256 devices in a mesh: grp: 2 (over y), dp: 128 (over z, x, core).
Axes of the slice: x: 4, y: 2, z: 16, core: 2. Of those that a mesh axis runs over, the one named last changes fastest.
The devices are a block of a 4x16x16 slice.
Arguments:
- hidden_in: bfloat16 [2, 512, 4096], P(None, ('grp', 'dp')), parts along dimension 1, may hold values from -6 to 6
- norm_gain: float32 [4096], replicated, may hold values from 0.1 to 1.9
- queries: bfloat16 [2, 512, 4096], P(None, ('grp', 'dp')), parts along dimension 1, may hold values from -72 to 72
- new_keys: bfloat16 [2, 512, 1024], P(None, ('grp', 'dp')), parts along dimension 1, may hold values from -9 to 9
- new_values: bfloat16 [2, 512, 1024], P(None, ('grp', 'dp')), parts along dimension 1, may hold values from -6 to 6
- cache_keys: bfloat16 [512, 384, 1024], P(('grp', 'dp')), parts along dimension 0, may hold values from -9 to 9
- cache_values: bfloat16 [512, 384, 1024], P(('grp', 'dp')), parts along dimension 0, may hold values from -6 to 6
- lengths: int32 [512], P(('grp', 'dp')), parts along dimension 0, may hold values from 1 to 384
- routes: int32 [2, 512, 2], P(None, ('grp', 'dp')), parts along dimension 1, may hold values from 0 to 3, all different within a row; in each aligned block of 2 rows (0 to 1, 2 to 3, ..., all dimensions but the last counted through in order) at most 2 rows name the same one
- gate_logits: float32 [2, 512, 2], P(None, ('grp', 'dp')), parts along dimension 1, may hold values from -6 to 6
- w_gate: bfloat16 [28672, 4096], P('dp'), may hold values from -0.09375 to 0.09375
- w_up: bfloat16 [28672, 4096], P('dp'), may hold values from -0.09375 to 0.09375
- w_down: bfloat16 [28672, 4096], P('dp'), may hold values from -0.0625 to 0.0625
Outputs:
- hidden_out: bfloat16 [2, 512, 4096], P(None, ('grp', 'dp')), parts along dimension 1
The draws below stay inside these ranges and needn't reach their ends.
There are 2 independent parts, one for each index of `grp`. The reference program is written for one: setup_inputs(seed, part) draws one part's arguments, and reference() takes and returns one part's arrays. A program takes and returns all parts, laid end to end along the dimension named above; an argument that names none is the same for every part. Nothing has to cross between parts.
Inputs may be any that keep to these rules, and one draw needn't show every extreme that they name: `routes`: each token names 2 different experts. Among the 2 tokens of one device at one decoded position no expert is named more than 2 times, a bound that some block reaches.
All inputs are finite; a program needn't handle non-finite values.
Results may differ from the reference program's by a relative error of at most 0.0055.
Values may be sent and summed in bfloat16 or wider, within the bound.
A program may use at most 192 MiB of HBM per device.

```python
import math
import jax
import jax.numpy as jnp
import numpy as np
from jax import lax

D = 4096
HEADS = 32
KV_HEADS = 8
HEAD_DIM = 128
TOP = 2
EXPERTS = 4
FFW = 7168
NEW = 2
DOC_DEV = 2
CACHE = 384
DOCS = 256
GROUP = 4
KV_WIDTH = 1024
CAP = 2


def key_fields(key):
    cached = jnp.clip(jax.random.normal(jax.random.fold_in(key, 101), (DOCS, CACHE, KV_HEADS * HEAD_DIM), jnp.float32), -5.0, 5.0)
    fresh = jnp.clip(jax.random.normal(jax.random.fold_in(key, 102), (NEW, DOCS, KV_HEADS * HEAD_DIM), jnp.float32), -5.0, 5.0)
    return (cached, fresh)


def draw_cache_keys(key, part):
    cached, fresh = key_fields(key)
    return cached.astype(jnp.bfloat16)


def draw_new_keys(key, part):
    cached, fresh = key_fields(key)
    return fresh.astype(jnp.bfloat16)


def draw_queries(key, part):
    drawn = jnp.clip(jax.random.normal(jax.random.fold_in(key, 104), (NEW, DOCS, HEADS * HEAD_DIM), jnp.float32), -5.0, 5.0)
    return drawn.astype(jnp.bfloat16)


def touch_ends(values, own_key, low, high):
    shape = values.shape
    index_at = [jax.random.randint(jax.random.fold_in(own_key, axis), (), 0, shape[axis]) for axis in range(len(shape))]
    values = values.at[tuple(index_at)].set(low)
    longest = shape.index(max(shape))
    index_at[longest] = (index_at[longest] + 1) % shape[longest]
    return values.at[tuple(index_at)].set(high)


def steps_of(key, extent, shards, low, top_value):
    def one(axis_at, parts):
        steps = jax.random.uniform(jax.random.fold_in(jax.random.fold_in(key, 6), axis_at), (parts,), jnp.float32, low / len(shards), top_value / len(shards))
        return jnp.repeat(jnp.exp(steps), extent[axis_at] // parts).reshape((-1,) + (1,) * (len(extent) - axis_at - 1))

    loudness = one(*shards[0])
    for cut in shards[1:]:
        loudness = loudness * one(*cut)
    return loudness


def routed_block(own_key, own, number, rows, amount, top, most, lean):
    sequence = jax.random.permutation(own_key, amount)
    crowded, common = load_shares(amount, rows * top, most, lean, True), load_shares(amount, rows * top, most, lean, False)
    places = jnp.arange(amount)

    def named(sizes, turn):
        used = int((sizes > 0).sum())
        fixed = max(1, used // 4)
        passed = fixed + (places - fixed + turn * (used - fixed)) % max(1, amount - fixed)
        return jnp.zeros((amount,), jnp.int32).at[sequence[jnp.where(places < fixed, places, passed)]].set(jnp.asarray(sizes, jnp.int32))

    sizes = jnp.where(number % 4 == 0, named(crowded, number // 4), named(common, number - number // 4 - 1))
    mixed = jax.random.permutation(jax.random.fold_in(own, 3), amount)
    source_of, taker = mixed[0:amount // 2 * 2:2], mixed[1:amount // 2 * 2:2]
    margin = jnp.minimum(sizes[source_of] - 1, most - sizes[taker]) // 2
    margin = jnp.where((source_of == sequence[0]) | (taker == sequence[0]) | (sizes[taker] == 0), 0, jnp.maximum(margin, 0))
    passed = jax.random.randint(jax.random.fold_in(own, 4), (amount // 2,), 0, 1 << 20) % (margin + 1)
    sizes = sizes.at[source_of].add(-passed).at[taker].add(passed)
    labels = jnp.searchsorted(jnp.cumsum(sizes), jnp.arange(rows * top), side="right").astype(jnp.int32)
    table = labels.reshape(top, rows).T
    table = table[jax.random.permutation(jax.random.fold_in(own, 1), rows)]
    turn = jax.random.randint(jax.random.fold_in(own, 2), (rows, 1), 0, top)
    return jnp.take_along_axis(table, (jnp.arange(top)[None, :] + turn) % top, axis=1)


def load_shares(amount, total, limit, lean, full):
    weights = [(1 << 20) // math.isqrt(grade ** lean) + 1 for grade in range(1, amount + 1)]
    largest = limit if full else min(limit, max(-(-total // amount), total * weights[0] // sum(weights)))
    least = 1 if total - largest >= amount - 1 else 0
    holding, spare = [largest] + [least] * (amount - 1), total - largest - least * (amount - 1)
    while spare > 0:
        free = [i for i in range(1, amount) if holding[i] < largest] or [i for i in range(1, amount) if holding[i] < limit]
        whole, budget = sum([weights[i] for i in free]), spare
        for i in free:
            more = min(limit - holding[i], max(1, budget * weights[i] // whole), spare)
            holding[i] = holding[i] + more
            spare = spare - more
    return np.array(holding)


def gaussian(key, dims, scale, most, shards=(), kind=jnp.bfloat16):
    values = jax.random.normal(key, dims, jnp.float32) * scale
    if len(shards) > 0:
        values = steps_of(key, dims, shards, -0.22, 0.18) * values
    return jnp.clip(values, min=-most, max=most).astype(kind)


def setup_inputs(seed: int = 0, part: int = 0) -> dict:
    arg_keys = jax.random.split(jax.random.key(seed), 14)
    part_keys = jax.random.split(jax.random.fold_in(arg_keys[13], part), 14)
    hidden_in = gaussian(part_keys[0], (NEW, DOCS, D), 1.0, 6.0, ((1, 128),))
    norm_gain = jnp.clip(1.0 + 0.18 * jax.random.normal(arg_keys[1], (D,), jnp.float32), 0.1, 1.9)
    queries = draw_queries(jax.random.fold_in(jax.random.fold_in(arg_keys[13], part), 71), part)
    new_keys = draw_new_keys(jax.random.fold_in(jax.random.fold_in(arg_keys[13], part), 71), part)
    new_values = gaussian(part_keys[4], (NEW, DOCS, KV_WIDTH), 1.0, 6.0, ((1, 128),))
    cache_keys = draw_cache_keys(jax.random.fold_in(jax.random.fold_in(arg_keys[13], part), 71), part)
    cache_values = gaussian(part_keys[6], (DOCS, CACHE, KV_WIDTH), 1.0, 6.0, ((0, 128),))
    lengths = touch_ends(jax.random.randint(part_keys[7], (DOCS,), 1, CACHE + 1), jax.random.fold_in(part_keys[7], 1), 1, CACHE).astype(jnp.int32)
    routes_keys = jax.random.split(jax.random.fold_in(part_keys[8], 1), NEW * DOCS // DOC_DEV)
    routes_turns = jax.random.permutation(jax.random.fold_in(part_keys[8], 3), NEW * DOCS // DOC_DEV)
    routes = jax.vmap(lambda own, number: routed_block(jax.random.fold_in(part_keys[8], 2), own, number, DOC_DEV, EXPERTS, TOP, CAP, 2))(routes_keys, routes_turns).reshape((NEW, DOCS, TOP))
    gate_logits = gaussian(part_keys[9], (NEW, DOCS, TOP), 1.5, 6.0, ((1, 128),), jnp.float32)
    w_gate = gaussian(arg_keys[10], (EXPERTS * FFW, D), D ** -0.5, 0.09375, ((0, 128),))
    w_up = gaussian(arg_keys[11], (EXPERTS * FFW, D), D ** -0.5, 0.09375, ((0, 128),))
    w_down = gaussian(arg_keys[12], (EXPERTS * FFW, D), FFW ** -0.5, 0.0625, ((0, 128),))
    return {"hidden_in": hidden_in, "norm_gain": norm_gain, "queries": queries, "new_keys": new_keys, "new_values": new_values, "cache_keys": cache_keys, "cache_values": cache_values, "lengths": lengths, "routes": routes, "gate_logits": gate_logits, "w_gate": w_gate, "w_up": w_up, "w_down": w_down}


def attend(queries, new_keys, new_values, cache_keys, cache_values, lengths):
    docs = queries.shape[1]
    cache_len = cache_keys.shape[1]
    score_scale = HEAD_DIM ** (-0.5)
    query_heads = queries.astype(jnp.float32).reshape(NEW, docs, KV_HEADS, GROUP, HEAD_DIM)
    keys_cache = cache_keys.astype(jnp.float32).reshape(docs, cache_len, KV_HEADS, HEAD_DIM)
    vals_cache = cache_values.astype(jnp.float32).reshape(docs, cache_len, KV_HEADS, HEAD_DIM)
    keys_fresh = new_keys.astype(jnp.float32).reshape(NEW, docs, KV_HEADS, HEAD_DIM)
    vals_fresh = new_values.astype(jnp.float32).reshape(NEW, docs, KV_HEADS, HEAD_DIM)
    scores_cache = jnp.einsum('tdhgc,dshc->tdhgs', query_heads, keys_cache) * score_scale
    scores_fresh = jnp.einsum('tdhgc,udhc->tdhgu', query_heads, keys_fresh) * score_scale
    positions = jnp.arange(cache_len, dtype=jnp.int32)
    in_range = positions[None, :] < lengths[:, None]
    scores_cache = jnp.where(in_range[None, :, None, None, :], scores_cache, -1e+30)
    order = jnp.arange(NEW, dtype=jnp.int32)
    causal = order[None, :] <= order[:, None]
    scores_fresh = jnp.where(causal[:, None, None, None, :], scores_fresh, -1e+30)
    largest = jnp.maximum(lax.optimization_barrier(jnp.max(scores_cache, -1, keepdims=True)), lax.optimization_barrier(jnp.max(scores_fresh, -1, keepdims=True)))
    exp_cache = jnp.exp(scores_cache - largest)
    exp_fresh = jnp.exp(scores_fresh - largest)
    total = lax.optimization_barrier(jnp.sum(exp_cache, -1, keepdims=True)) + lax.optimization_barrier(jnp.sum(exp_fresh, -1, keepdims=True))
    probs_cache = (exp_cache / total).astype(jnp.bfloat16).astype(jnp.float32)
    probs_fresh = (exp_fresh / total).astype(jnp.bfloat16).astype(jnp.float32)
    context = jnp.einsum('tdhgs,dshc->tdhgc', probs_cache, vals_cache)
    context = context + jnp.einsum('tdhgu,udhc->tdhgc', probs_fresh, vals_fresh)
    return context.reshape(NEW, docs, HEADS * HEAD_DIM)

def reference(hidden_in, norm_gain, queries, new_keys, new_values, cache_keys, cache_values, lengths, routes, gate_logits, w_gate, w_up, w_down):
    context = attend(queries, new_keys, new_values, cache_keys, cache_values, lengths)
    carried = hidden_in.astype(jnp.float32) + context
    normed = (carried * lax.rsqrt(lax.optimization_barrier(jnp.mean(carried * carried, -1, keepdims=True)) + 1e-05) * norm_gain).astype(jnp.bfloat16)
    flat_rows = normed.reshape(NEW * DOCS, D)
    flat_routes = routes.reshape(NEW * DOCS, TOP)
    flat_logits = gate_logits.reshape(NEW * DOCS, TOP)
    top_share = jax.nn.sigmoid(flat_logits[:, 0] - flat_logits[:, 1])
    shares = jnp.stack([top_share, 1.0 - top_share], axis=1)
    result = carried.reshape(NEW * DOCS, D)
    for expert in range(EXPERTS):
        weight_rows = lax.optimization_barrier(jnp.sum(shares * (flat_routes == expert).astype(jnp.float32), axis=1))
        gate_block = w_gate[expert * FFW:(expert + 1) * FFW]
        up_block = w_up[expert * FFW:(expert + 1) * FFW]
        down_block = w_down[expert * FFW:(expert + 1) * FFW]
        gate_val = lax.dot_general(flat_rows, gate_block, (((1,), (1,)), ((), ())), preferred_element_type=jnp.float32)
        up_val = lax.dot_general(flat_rows, up_block, (((1,), (1,)), ((), ())), preferred_element_type=jnp.float32)
        act = (jax.nn.silu(gate_val) * up_val).astype(jnp.bfloat16)
        expert_out = jnp.dot(act, down_block, preferred_element_type=jnp.float32)
        result = result + weight_rows[:, None] * expert_out
    return result.reshape(NEW, DOCS, D).astype(jnp.bfloat16)
```

```python
import jax
import jax.numpy as jnp
from jax import lax
from jax.sharding import PartitionSpec as P

HEADS = 32
KV_HEADS = 8
HEAD_DIM = 128
EXPERTS = 4
NEW = 2
RS_TYPE = jnp.bfloat16


def attend(queries, new_keys, new_values, cache_keys, cache_values, lengths):
    docs = queries.shape[1]
    cache_len = cache_keys.shape[1]
    group_size = HEADS // KV_HEADS
    score_scale = HEAD_DIM ** (-0.5)
    query_heads = queries.reshape(NEW, docs, KV_HEADS, group_size, HEAD_DIM)
    keys_cache = cache_keys.reshape(docs, cache_len, KV_HEADS, HEAD_DIM)
    vals_cache = cache_values.reshape(docs, cache_len, KV_HEADS, HEAD_DIM)
    keys_fresh = new_keys.reshape(NEW, docs, KV_HEADS, HEAD_DIM)
    vals_fresh = new_values.reshape(NEW, docs, KV_HEADS, HEAD_DIM)
    scores_cache = (
        jnp.einsum("tdhgc,dshc->tdhgs", query_heads, keys_cache, preferred_element_type=jnp.float32)
        * score_scale
    )
    scores_fresh = (
        jnp.einsum("tdhgc,udhc->tdhgu", query_heads, keys_fresh, preferred_element_type=jnp.float32)
        * score_scale
    )
    positions = jnp.arange(cache_len, dtype=jnp.int32)
    in_range = positions[None, :] < lengths[:, None]
    scores_cache = jnp.where(in_range[None, :, None, None, :], scores_cache, -1e30)
    order = jnp.arange(NEW, dtype=jnp.int32)
    causal = order[None, :] <= order[:, None]
    scores_fresh = jnp.where(causal[:, None, None, None, :], scores_fresh, -1e30)
    largest = jnp.maximum(
        jnp.max(scores_cache, -1, keepdims=True), jnp.max(scores_fresh, -1, keepdims=True)
    )
    exp_cache = jnp.exp(scores_cache - largest)
    exp_fresh = jnp.exp(scores_fresh - largest)
    total = jnp.sum(exp_cache, -1, keepdims=True) + jnp.sum(exp_fresh, -1, keepdims=True)
    probs_cache = (exp_cache / total).astype(jnp.bfloat16)
    probs_fresh = (exp_fresh / total).astype(jnp.bfloat16)
    context = jnp.einsum(
        "tdhgs,dshc->tdhgc", probs_cache, vals_cache, preferred_element_type=jnp.float32
    )
    context = context + jnp.einsum(
        "tdhgu,udhc->tdhgc", probs_fresh, vals_fresh, preferred_element_type=jnp.float32
    )
    return context.reshape(NEW, docs, HEADS * HEAD_DIM)


def expert_rows(flat_rows, row_weight, w_gate, w_up, w_down):
    gate_val = lax.dot_general(
        flat_rows, w_gate, (((1,), (1,)), ((), ())), preferred_element_type=jnp.float32
    )
    up_val = lax.dot_general(
        flat_rows, w_up, (((1,), (1,)), ((), ())), preferred_element_type=jnp.float32
    )
    act = (jax.nn.silu(gate_val) * up_val * row_weight).astype(jnp.bfloat16)
    return jnp.dot(act, w_down, preferred_element_type=jnp.float32)


def per_device(
    hidden_in,
    norm_gain,
    queries,
    new_keys,
    new_values,
    cache_keys,
    cache_values,
    lengths,
    routes,
    gate_logits,
    w_gate,
    w_up,
    w_down,
):
    docs = hidden_in.shape[1]
    width = hidden_in.shape[2]
    context = attend(queries, new_keys, new_values, cache_keys, cache_values, lengths)
    carried = hidden_in.astype(jnp.float32) + context
    normed = (
        carried * lax.rsqrt(jnp.mean(carried * carried, -1, keepdims=True) + 1e-05) * norm_gain
    ).astype(jnp.bfloat16)
    top_share = jax.nn.sigmoid(gate_logits[..., 0] - gate_logits[..., 1])
    shares = jnp.stack([top_share, 1.0 - top_share], axis=-1)
    experts = jnp.arange(EXPERTS, dtype=jnp.int32)
    named = (routes[..., None] == experts).astype(jnp.float32)
    weights = jnp.sum(shares[..., None] * named, axis=2)
    rows = NEW * docs
    devices = lax.axis_size("dp")
    mine = lax.axis_index("dp") // (devices // EXPERTS)
    all_rows = lax.all_gather(normed.reshape(rows, width), "dp", axis=0, tiled=True)
    all_weights = lax.all_gather(weights.reshape(rows, EXPERTS), "dp", axis=0, tiled=True)
    my_weight = jnp.sum(
        jnp.where(experts[None, :] == mine, all_weights, 0.0), axis=1, keepdims=True
    )
    partial_value = expert_rows(all_rows, my_weight, w_gate, w_up, w_down)
    summed = lax.psum_scatter(
        partial_value.astype(RS_TYPE), "dp", scatter_dimension=0, tiled=True
    )
    result = carried.reshape(rows, width) + summed.astype(jnp.float32)
    return result.astype(jnp.bfloat16).reshape(NEW, docs, width)


def solution(mesh):
    in_specs = (
        P(None, ("grp", "dp"), None),
        P(),
        P(None, ("grp", "dp"), None),
        P(None, ("grp", "dp"), None),
        P(None, ("grp", "dp"), None),
        P(("grp", "dp"), None, None),
        P(("grp", "dp"), None, None),
        P(("grp", "dp")),
        P(None, ("grp", "dp"), None),
        P(None, ("grp", "dp"), None),
        P("dp", None),
        P("dp", None),
        P("dp", None),
    )
    out_specs = P(None, ("grp", "dp"), None)
    return jax.shard_map(
        per_device, mesh=mesh, in_specs=in_specs, out_specs=out_specs, check_vma=False
    )
```

```python
import functools

import jax
import jax.numpy as jnp
from jax import lax
from jax.experimental import pallas as pl
from jax.experimental.pallas import tpu as pltpu
from jax.sharding import PartitionSpec as P

HEADS = 32
KV_HEADS = 8
HEAD_DIM = 128
EXPERTS = 4
NEW = 2
DOC_DEV = 2
ROWS = NEW * DOC_DEV
EXT = 128
TAIL = 128
XS = 4
CORES = 2
MESH = pl.DeviceIdType.MESH
F32 = jnp.float32
BF16 = jnp.bfloat16


def attend_kernel(
    hid_ref, gain_ref, q_ref, nk_ref, nv_ref, ck_ref, cv_ref, len_ref, ext_ref,
    pay_ref, carried_ref, kbuf, vbuf, sems,
):
    docs, cache_len, kv_width = ck_ref.shape
    copies = []
    for d in range(docs):
        for i, (src, dst) in enumerate(((ck_ref, kbuf), (cv_ref, vbuf))):
            copy = pltpu.make_async_copy(
                src.at[d], dst.at[d, pl.ds(0, cache_len)], sems.at[d, i]
            )
            copy.start()
            copies.append(copy)
    q_all = q_ref[...].astype(F32)
    nk_all = nk_ref[...].astype(F32)
    nv_all = nv_ref[...].astype(F32)
    hid_all = hid_ref[...].astype(F32)
    span = cache_len + TAIL
    rows = HEADS * NEW
    per_kv = rows // KV_HEADS
    col = lax.broadcasted_iota(jnp.int32, (rows, span), 1)
    row_at = lax.broadcasted_iota(jnp.int32, (rows, span), 0)
    fresh_ok = (col == cache_len) | ((col == cache_len + 1) & (row_at % NEW == 1))
    block = (
        lax.broadcasted_iota(jnp.int32, (rows, kv_width), 0) // per_kv
        == lax.broadcasted_iota(jnp.int32, (rows, kv_width), 1) // HEAD_DIM
    )
    zeros = jnp.zeros((TAIL - NEW, kv_width), F32)
    parts = []
    for d in range(docs):
        kbuf[d, cache_len:, :] = jnp.concatenate([nk_all[:, d, :], zeros], axis=0).astype(BF16)
        vbuf[d, cache_len:, :] = jnp.concatenate([nv_all[:, d, :], zeros], axis=0).astype(BF16)
        q_doc = q_all[:, d, :]
        q_rows = jnp.concatenate(
            [q_doc[:, h * HEAD_DIM : (h + 1) * HEAD_DIM] for h in range(HEADS)], axis=0
        )
        q_block = jnp.where(block, jnp.concatenate([q_rows] * KV_HEADS, axis=1), 0.0).astype(BF16)
        copies[2 * d].wait()
        scores = lax.dot_general(
            q_block, kbuf[d], (((1,), (1,)), ((), ())), preferred_element_type=F32
        ) * (HEAD_DIM ** (-0.5))
        keep = (col < len_ref[d]) | fresh_ok
        scores = jnp.where(keep, scores, -1e30)
        e = jnp.exp(scores - jnp.max(scores, -1, keepdims=True))
        probs = (e / jnp.sum(e, -1, keepdims=True)).astype(BF16)
        copies[2 * d + 1].wait()
        out = jnp.dot(probs, vbuf[d], preferred_element_type=F32)
        pieces = []
        for h in range(HEADS):
            kv = h * NEW // per_kv
            pieces.append(out[h * NEW : (h + 1) * NEW, kv * HEAD_DIM : (kv + 1) * HEAD_DIM])
        parts.append(hid_all[:, d, :] + jnp.concatenate(pieces, axis=1))
    carried = jnp.concatenate(parts, axis=0)
    carried_ref[...] = carried
    width = carried.shape[1]
    normed = carried * lax.rsqrt(jnp.mean(carried * carried, -1, keepdims=True) + 1e-05)
    pay_ref[:, :width] = (normed * gain_ref[...]).astype(BF16)
    pay_ref[:, width:] = ext_ref[...].astype(BF16)


def attention(hidden_in, norm_gain, queries, new_keys, new_values, cache_keys, cache_values, lengths, ext):
    docs, cache_len, kv_width = cache_keys.shape
    width = hidden_in.shape[2]
    vmem = pl.BlockSpec(memory_space=pltpu.VMEM)
    hbm = pl.BlockSpec(memory_space=pl.ANY)
    return pl.pallas_call(
        attend_kernel,
        name="attend",
        out_shape=(
            jax.ShapeDtypeStruct((ROWS, width + EXT), BF16),
            jax.ShapeDtypeStruct((ROWS, width), F32),
        ),
        in_specs=[vmem, vmem, vmem, vmem, vmem, hbm, hbm, pl.BlockSpec(memory_space=pltpu.SMEM), vmem],
        out_specs=(vmem, vmem),
        scratch_shapes=[
            pltpu.VMEM((docs, cache_len + TAIL, kv_width), BF16),
            pltpu.VMEM((docs, cache_len + TAIL, kv_width), BF16),
            pltpu.SemaphoreType.DMA((docs, 2)),
        ],
    )(hidden_in, norm_gain.reshape(1, width), queries, new_keys, new_values, cache_keys, cache_values, lengths, ext)


def experts_kernel(
    nz, pay_ref, carried_ref, wg_ref, wu_ref, wd_ref, out_ref,
    wg, wu, wd, xin, rows, mine, pair_out, pair_in, ring_out, ring_in, xs_out, xs_in,
    w_sems, xg_send, xg_recv, ag_send, ag_recv, d2_send, d2_recv,
    pr_send, pr_recv, rs_send, rs_recv, xs_send, xs_recv,
):
    me = lax.axis_index("dp")
    core = me % CORES
    x = (me // CORES) % XS
    z = me // (CORES * XS)
    half = nz // 2
    width = carried_ref.shape[1]
    full = width + EXT
    class_rows = XS * ROWS
    slabs_per_expert = nz // EXPERTS
    mine_expert = z // slabs_per_expert

    def at(zz, xx, cc):
        return {"dp": (zz * XS + xx) * CORES + cc}

    def slab_of(offset):
        return lax.rem(z + offset + nz, nz)

    partner = at(z, x, 1 - core)
    step_to = (at(slab_of(1), x, core), at(slab_of(-1), x, core))
    x_peers = [lax.rem(x + k, XS) for k in range(1, XS)]

    w_copies = [
        pltpu.make_async_copy(src, dst, w_sems.at[i])
        for i, (src, dst) in enumerate(((wg_ref, wg), (wu_ref, wu), (wd_ref, wd)))
    ]
    for copy in w_copies:
        copy.start()

    barrier = pltpu.get_barrier_semaphore()
    greeted = [partner, step_to[0], step_to[1]] + [at(z, p, core) for p in x_peers]
    for device in greeted:
        pl.semaphore_signal(barrier, inc=1, device_id=device, device_id_type=MESH)
    pl.semaphore_wait(barrier, len(greeted))

    def remote(src, dst, send, recv, device):
        return pltpu.make_async_remote_copy(
            src_ref=src, dst_ref=dst, send_sem=send, recv_sem=recv,
            device_id=device, device_id_type=MESH,
        )

    xg = [
        remote(pay_ref, xin.at[x], xg_send.at[k], xg_recv.at[k], at(z, p, core))
        for k, p in enumerate(x_peers)
    ]
    for copy in xg:
        copy.start()
    xin[x] = pay_ref[...]
    for copy in xg:
        copy.wait_recv()
    rows[z, 0] = jnp.concatenate([xin[j].astype(F32) for j in range(XS)], axis=0).astype(BF16)

    tiles = full // 128
    cuts = [tiles * i // 4 * 128 for i in range(5)]
    ag_cuts = [pl.ds(cuts[i], cuts[i + 1] - cuts[i]) for i in range(4)]
    sides = ((0, -1), (1, 1))

    def ag_copy(way, sign, s, p):
        ref = rows.at[slab_of(sign * s), 0, :, ag_cuts[p]]
        return remote(ref, ref, ag_send.at[way, s, p], ag_recv.at[way, s, p], step_to[way])

    def d2_copy(way, sign, s):
        slab = slab_of(sign * s)
        return remote(
            rows.at[slab, 0], rows.at[slab, 1], d2_send.at[way, s], d2_recv.at[way, s], partner
        )

    def last_pieces(way):
        return (0, 1) if way == 0 else (2, 3)

    for p in range(4):
        for way, sign in sides:
            ag_copy(way, sign, 0, p).start()
    d2_copy(0, -1, 0).start()

    def gather_step(s, carry):
        for p in range(4):
            for way, sign in sides:
                ag_copy(way, sign, s - 1, p).wait_recv()
                ag_copy(way, sign, s, p).start()
        for way, sign in sides:
            d2_copy(way, sign, s).start()
        return carry

    lax.fori_loop(1, half - 1, gather_step, 0)
    for p in range(4):
        for way, sign in sides:
            ag_copy(way, sign, half - 2, p).wait_recv()
            if p in last_pieces(way):
                ag_copy(way, sign, half - 1, p).start()
    for way, sign in sides:
        d2_copy(way, sign, half - 1).start()
    for way, sign in sides:
        for p in last_pieces(way):
            ag_copy(way, sign, half - 1, p).wait_recv()
    d2_copy(0, -1, half).start()
    for copy in w_copies:
        copy.wait()

    nt = (((1,), (1,)), ((), ()))
    quarter = width // 4

    def expert_rows(offsets, out_way):
        slabs = [slab_of(o) for o in offsets]
        lhs = jnp.concatenate([rows[w, k, :, :width] for w in slabs for k in range(2)], axis=0)
        ext = jnp.concatenate([rows[w, k, :, width:] for w in slabs for k in range(2)], axis=0)
        lane = lax.broadcasted_iota(jnp.int32, ext.shape, 1)
        chosen = (lane == mine_expert) | (lane == mine_expert + EXPERTS)
        weight = jnp.sum(jnp.where(chosen, ext.astype(F32), 0.0), axis=-1, keepdims=True)
        gate = lax.dot_general(lhs, wg[...], nt, preferred_element_type=F32)
        up = lax.dot_general(lhs, wu[...], nt, preferred_element_type=F32)
        act = (jax.nn.silu(gate) * up * weight).astype(BF16)
        for q in range(4):
            cut = slice(q * quarter, (q + 1) * quarter)
            value = jnp.dot(act, wd[:, cut], preferred_element_type=F32)
            for i, w in enumerate(slabs):
                base = 2 * i * class_rows
                mine[w, :, cut] = value[base : base + class_rows]
                pair_out[w, :, cut] = value[base + class_rows : base + 2 * class_rows].astype(BF16)

    def pair_copy(way, offset_abs):
        slab = slab_of(-offset_abs if way == 0 else offset_abs)
        return remote(
            pair_out.at[slab], pair_in.at[slab], pr_send.at[way, offset_abs],
            pr_recv.at[way, offset_abs], partner,
        )

    def d2_wait(way, s):
        d2_copy(way, -1 if way == 0 else 1, s).wait_recv()

    def rs_copy(way, d, p):
        cut = pl.ds(p * quarter, quarter)
        return remote(
            ring_out.at[way, d - 1, :, cut], ring_in.at[way, d - 1, :, cut],
            rs_send.at[way, d - 1, p], rs_recv.at[way, d - 1, p], step_to[way],
        )

    def local_sum(slab, p):
        cut = slice(p * quarter, (p + 1) * quarter)
        return mine[slab, :, cut] + pair_in[slab, :, cut].astype(F32)

    def pass_on(d, has_input):
        for p in range(4):
            for way in range(2):
                cut = slice(p * quarter, (p + 1) * quarter)
                total = local_sum(slab_of(d if way == 0 else -d), p)
                if has_input(way, p):
                    rs_copy(way, d + 1, p).wait_recv()
                    total = total + ring_in[way, d, :, cut].astype(F32)
                ring_out[way, d - 1, :, cut] = total.astype(BF16)
                rs_copy(way, d, p).start()

    d2_wait(1, half - 1)
    d2_wait(0, half - 1)
    d2_wait(0, half)
    expert_rows([half], 0)
    pair_copy(0, half).start()
    expert_rows([half - 1, 1 - half], 0)
    pair_copy(0, half - 1).start()
    pair_copy(1, half - 1).start()
    pair_copy(0, half).wait_recv()
    for way in range(2):
        for p in last_pieces(way):
            cut = slice(p * quarter, (p + 1) * quarter)
            ring_out[way, half - 1, :, cut] = local_sum(slab_of(half), p).astype(BF16)
            rs_copy(way, half, p).start()

    def next_rows(d):
        d2_wait(0, d)
        d2_wait(1, d)
        expert_rows([d, -d], 0)
        pair_copy(0, d).start()
        pair_copy(1, d).start()

    def take_pairs(d):
        pair_copy(0, d).wait_recv()
        pair_copy(1, d).wait_recv()

    next_rows(half - 2)
    take_pairs(half - 1)
    pass_on(half - 1, lambda way, p: p in last_pieces(way))

    def sum_step(i, carry):
        d = half - 2 - i
        next_rows(d - 1)
        take_pairs(d)
        pass_on(d, lambda way, p: True)
        return carry

    lax.fori_loop(0, half - 3, sum_step, 0)
    d2_wait(0, 0)
    expert_rows([0], 0)
    pair_copy(0, 0).start()
    take_pairs(1)
    pass_on(1, lambda way, p: True)

    pair_copy(0, 0).wait_recv()
    for p in range(4):
        cut = slice(p * quarter, (p + 1) * quarter)
        total = local_sum(z, p)
        for way in range(2):
            rs_copy(way, 1, p).wait_recv()
            total = total + ring_in[way, 0, :, cut].astype(F32)
        for j in range(XS):
            xs_out[j, :, cut] = total[j * ROWS : (j + 1) * ROWS].astype(BF16)
    xs = [
        remote(xs_out.at[p], xs_in.at[k], xs_send.at[k], xs_recv.at[k], at(z, p, core))
        for k, p in enumerate(x_peers)
    ]
    for copy in xs:
        copy.start()
    result = carried_ref[...] + xs_out[x].astype(F32)
    for k, copy in enumerate(xs):
        copy.wait_recv()
        result = result + xs_in[k].astype(F32)
    for d in range(DOC_DEV):
        for t in range(NEW):
            r = d * NEW + t
            out_ref[t, d : d + 1, :] = result[r : r + 1].astype(BF16)

    for copy in xg + xs:
        copy.wait_send()

    def drain(s, carry):
        for p in range(4):
            for way, sign in sides:
                ag_copy(way, sign, s, p).wait_send()
                rs_copy(way, s + 1, p).wait_send()
        for way, sign in sides:
            d2_copy(way, sign, s + 1).wait_send()
            pair_copy(way, s + 1).wait_send()
        return carry

    lax.fori_loop(0, half - 1, drain, 0)
    for way, sign in sides:
        for p in last_pieces(way):
            ag_copy(way, sign, half - 1, p).wait_send()
            rs_copy(way, half, p).wait_send()
    for s in (0, half):
        d2_copy(0, -1, s).wait_send()
        pair_copy(0, s).wait_send()


def experts(payload, carried, w_gate, w_up, w_down, nz):
    width = carried.shape[1]
    hidden = w_gate.shape[0]
    half = nz // 2
    class_rows = XS * ROWS
    vmem = pl.BlockSpec(memory_space=pltpu.VMEM)
    hbm = pl.BlockSpec(memory_space=pl.ANY)
    dma = pltpu.SemaphoreType.DMA
    return pl.pallas_call(
        functools.partial(experts_kernel, nz),
        name="experts",
        out_shape=jax.ShapeDtypeStruct((NEW, DOC_DEV, width), BF16),
        in_specs=[vmem, vmem, hbm, hbm, hbm],
        out_specs=vmem,
        scratch_shapes=[
            pltpu.VMEM((hidden, width), BF16),
            pltpu.VMEM((hidden, width), BF16),
            pltpu.VMEM((hidden, width), BF16),
            pltpu.VMEM((XS, ROWS, width + EXT), BF16),
            pltpu.VMEM((nz, 2, class_rows, width + EXT), BF16),
            pltpu.VMEM((nz, class_rows, width), F32),
            pltpu.VMEM((nz, class_rows, width), BF16),
            pltpu.VMEM((nz, class_rows, width), BF16),
            pltpu.VMEM((2, half, class_rows, width), BF16),
            pltpu.VMEM((2, half, class_rows, width), BF16),
            pltpu.VMEM((XS, ROWS, width), BF16),
            pltpu.VMEM((XS - 1, ROWS, width), BF16),
            dma((3,)),
            dma((XS - 1,)), dma((XS - 1,)),
            dma((2, half, 4)), dma((2, half, 4)),
            dma((2, half + 1)), dma((2, half + 1)),
            dma((2, half + 1)), dma((2, half + 1)),
            dma((2, half, 4)), dma((2, half, 4)),
            dma((XS - 1,)), dma((XS - 1,)),
        ],
        compiler_params=pltpu.CompilerParams(
            collective_id=0, has_side_effects=True, vmem_limit_bytes=56 * 1024 * 1024
        ),
    )(payload, carried, w_gate, w_up, w_down)


def per_device(
    hidden_in, norm_gain, queries, new_keys, new_values, cache_keys, cache_values,
    lengths, routes, gate_logits, w_gate, w_up, w_down,
):
    top_share = jax.nn.sigmoid(gate_logits[..., 0] - gate_logits[..., 1])
    shares = jnp.stack([top_share, 1.0 - top_share], axis=-1)
    lanes = jnp.arange(EXT, dtype=jnp.int32)
    weights = jnp.sum(shares[..., None] * (routes[..., None] == lanes % EXPERTS), axis=2)
    weights = jnp.swapaxes(weights, 0, 1).reshape(ROWS, EXT)
    high = lax.reduce_precision(weights, 8, 7)
    ext = jnp.where(lanes < EXPERTS, high, jnp.where(lanes < 2 * EXPERTS, weights - high, 0.0))
    payload, carried = attention(
        hidden_in, norm_gain, queries, new_keys, new_values, cache_keys, cache_values, lengths, ext
    )
    nz = lax.axis_size("dp") // (XS * CORES)
    return experts(payload, carried, w_gate, w_up, w_down, nz)


def solution(mesh):
    in_specs = (
        P(None, ("grp", "dp"), None),
        P(),
        P(None, ("grp", "dp"), None),
        P(None, ("grp", "dp"), None),
        P(None, ("grp", "dp"), None),
        P(("grp", "dp"), None, None),
        P(("grp", "dp"), None, None),
        P(("grp", "dp")),
        P(None, ("grp", "dp"), None),
        P(None, ("grp", "dp"), None),
        P("dp", None),
        P("dp", None),
        P("dp", None),
    )
    out_specs = P(None, ("grp", "dp"), None)
    return jax.shard_map(
        per_device, mesh=mesh, in_specs=in_specs, out_specs=out_specs, check_vma=False
    )
```

```python
import functools

import jax
import jax.numpy as jnp
from jax import lax
from jax.experimental import pallas as pl
from jax.experimental.pallas import tpu as pltpu
from jax.sharding import PartitionSpec as P

HEADS = 32
KV_HEADS = 8
HEAD_DIM = 128
EXPERTS = 4
NEW = 2
DOC_DEV = 2
ROWS = NEW * DOC_DEV
EXT = 128
TAIL = 128
XS = 4
PIECES = 4
CORES = 2
MESH = pl.DeviceIdType.MESH
F32 = jnp.float32
BF16 = jnp.bfloat16


def layer_kernel(
    nz, hid_hbm, gain_hbm, q_hbm, nk_hbm, nv_hbm, ck_hbm, cv_hbm, len_ref, routes_ref, logits_ref,
    wg_hbm, wu_hbm, wd_hbm, out_ref,
    hid, gain, q, nk, nv, kbuf, vbuf, wg, wu, wd, carried_ref,
    xin, rows, mine, pair_out, pair_in, ring_out, ring_in, xs_out, xs_in,
    in_sems, kv_sems, w_sems, xg_send, xg_recv, ag_send, ag_recv, d2_send, d2_recv,
    pr_send, pr_recv, rs_send, rs_recv, xs_send, xs_recv,
):
    me = lax.axis_index("dp")
    core = me % CORES
    x = (me // CORES) % XS
    z = me // (CORES * XS)
    half = nz // 2
    width = carried_ref.shape[1]
    full = width + EXT
    class_rows = XS * ROWS
    mine_expert = z // (nz // EXPERTS)
    docs, span, kv_width = kbuf.shape
    cache_len = span - TAIL

    def at(zz, xx, cc):
        return {"dp": (zz * XS + xx) * CORES + cc}

    def slab_of(offset):
        return lax.rem(z + offset + nz, nz)

    partner = at(z, x, 1 - core)
    step_to = (at(slab_of(1), x, core), at(slab_of(-1), x, core))
    x_peers = [lax.rem(x + k, XS) for k in range(1, XS)]

    barrier = pltpu.get_barrier_semaphore()
    greeted = [partner, step_to[0], step_to[1]] + [at(z, p, core) for p in x_peers]
    for device in greeted:
        pl.semaphore_signal(barrier, inc=1, device_id=device, device_id_type=MESH)

    small = [
        pltpu.make_async_copy(src, dst, in_sems.at[i])
        for i, (src, dst) in enumerate(
            ((q_hbm, q), (nk_hbm, nk), (nv_hbm, nv), (hid_hbm, hid), (gain_hbm, gain))
        )
    ]
    kv = [
        pltpu.make_async_copy(src.at[d], dst.at[d, pl.ds(0, cache_len)], kv_sems.at[d, i])
        for d in range(docs)
        for i, (src, dst) in enumerate(((ck_hbm, kbuf), (cv_hbm, vbuf)))
    ]
    w_copies = [
        pltpu.make_async_copy(src, dst, w_sems.at[i])
        for i, (src, dst) in enumerate(((wg_hbm, wg), (wu_hbm, wu), (wd_hbm, wd)))
    ]
    for copy in small[:3] + kv + small[3:] + w_copies:
        copy.start()

    heads_rows = HEADS * NEW
    per_kv = heads_rows // KV_HEADS
    col = lax.broadcasted_iota(jnp.int32, (heads_rows, span), 1)
    row_at = lax.broadcasted_iota(jnp.int32, (heads_rows, span), 0)
    fresh_ok = (col == cache_len) | ((col == cache_len + 1) & (row_at % NEW == 1))
    block = (
        lax.broadcasted_iota(jnp.int32, (heads_rows, kv_width), 0) // per_kv
        == lax.broadcasted_iota(jnp.int32, (heads_rows, kv_width), 1) // HEAD_DIM
    )
    zeros = jnp.zeros((TAIL - NEW, kv_width), F32)

    lane = lax.broadcasted_iota(jnp.int32, (ROWS, EXT), 1)
    at_row = lax.broadcasted_iota(jnp.int32, (ROWS, EXT), 0)

    def by_row(values):
        out = jnp.full((ROWS, EXT), values[0])
        for r in range(1, ROWS):
            out = jnp.where(at_row == r, values[r], out)
        return out

    order = [(t, d) for d in range(DOC_DEV) for t in range(NEW)]
    first = by_row([routes_ref[t, d, 0] for t, d in order])
    second = by_row([routes_ref[t, d, 1] for t, d in order])
    share = jax.nn.sigmoid(by_row([logits_ref[t, d, 0] - logits_ref[t, d, 1] for t, d in order]))
    expert_at = lane % EXPERTS
    weights = jnp.where(expert_at == first, share, 0.0) + jnp.where(
        expert_at == second, 1.0 - share, 0.0
    )
    high = weights.astype(BF16)
    low = (weights - high.astype(F32)).astype(BF16)
    zero_ext = jnp.zeros_like(high)
    ext = jnp.where(lane < EXPERTS, high, jnp.where(lane < 2 * EXPERTS, low, zero_ext))

    for copy in small[:3]:
        copy.wait()
    q_all = q[...].astype(F32)
    nk_all = nk[...].astype(F32)
    nv_all = nv[...].astype(F32)
    q_blocks = []
    for d in range(docs):
        kbuf[d, cache_len:, :] = jnp.concatenate([nk_all[:, d, :], zeros], axis=0).astype(BF16)
        vbuf[d, cache_len:, :] = jnp.concatenate([nv_all[:, d, :], zeros], axis=0).astype(BF16)
        q_doc = q_all[:, d, :]
        q_rows = jnp.concatenate(
            [q_doc[:, h * HEAD_DIM : (h + 1) * HEAD_DIM] for h in range(HEADS)], axis=0
        )
        q_blocks.append(
            jnp.where(block, jnp.concatenate([q_rows] * KV_HEADS, axis=1), 0.0).astype(BF16)
        )
    parts = []
    for d in range(docs):
        kv[2 * d].wait()
        scores = lax.dot_general(
            q_blocks[d], kbuf[d], (((1,), (1,)), ((), ())), preferred_element_type=F32
        ) * (HEAD_DIM ** (-0.5))
        keep = (col < len_ref[d]) | fresh_ok
        scores = jnp.where(keep, scores, -1e30)
        e = jnp.exp(scores - jnp.max(scores, -1, keepdims=True))
        probs = (e / jnp.sum(e, -1, keepdims=True)).astype(BF16)
        kv[2 * d + 1].wait()
        out = jnp.dot(probs, vbuf[d], preferred_element_type=F32)
        pieces = []
        for h in range(HEADS):
            k = h * NEW // per_kv
            pieces.append(out[h * NEW : (h + 1) * NEW, k * HEAD_DIM : (k + 1) * HEAD_DIM])
        parts.append(jnp.concatenate(pieces, axis=1))
    for copy in small[3:]:
        copy.wait()
    hid_all = hid[...].astype(F32)
    carried = jnp.concatenate([hid_all[:, d, :] + parts[d] for d in range(docs)], axis=0)
    carried_ref[...] = carried
    normed = carried * lax.rsqrt(jnp.mean(carried * carried, -1, keepdims=True) + 1e-05)
    xin[x, :, :width] = (normed * gain[...]).astype(BF16)
    xin[x, :, width:] = ext
    pl.semaphore_wait(barrier, len(greeted))

    def remote(src, dst, send, recv, device):
        return pltpu.make_async_remote_copy(
            src_ref=src, dst_ref=dst, send_sem=send, recv_sem=recv,
            device_id=device, device_id_type=MESH,
        )

    def whole(ref, send, recv):
        return remote(ref, ref, send, recv, partner)

    for p in x_peers:
        remote(xin.at[x], xin.at[x], xg_send.at[0], xg_recv.at[0], at(z, p, core)).start()
    xg_all = whole(xin.at[pl.ds(0, XS - 1)], xg_send.at[0], xg_recv.at[0])
    xg_all.wait_recv()
    rows[z, 0] = jnp.concatenate([xin[j].astype(F32) for j in range(XS)], axis=0).astype(BF16)

    tiles = full // 128
    cuts = [tiles * i // PIECES * 128 for i in range(PIECES + 1)]
    ag_cuts = [pl.ds(cuts[i], cuts[i + 1] - cuts[i]) for i in range(PIECES)]
    sides = ((0, -1), (1, 1))

    def ag_copy(way, sign, s, p, last=0):
        ref = rows.at[slab_of(sign * s), 0, :, ag_cuts[p]]
        return remote(ref, ref, ag_send.at[way, last], ag_recv.at[way, s, p], step_to[way])

    def d2_copy(way, sign, s):
        slab = slab_of(sign * s)
        return remote(rows.at[slab, 0], rows.at[slab, 1], d2_send.at[0], d2_recv.at[s], partner)

    def d2_wait(s, count):
        whole(rows.at[pl.ds(0, count), 1], d2_send.at[0], d2_recv.at[s]).wait_recv()

    def last_pieces(way):
        return tuple(range(PIECES // 2)) if way == 0 else tuple(range(PIECES // 2, PIECES))

    for p in range(PIECES):
        for way, sign in sides:
            ag_copy(way, sign, 0, p).start()
    d2_copy(0, -1, 0).start()

    def gather_step(s, carry):
        for p in range(PIECES):
            for way, sign in sides:
                ag_copy(way, sign, s - 1, p).wait_recv()
                ag_copy(way, sign, s, p).start()
        for way, sign in sides:
            d2_copy(way, sign, s).start()
        return carry

    nt = (((1,), (1,)), ((), ()))
    quarter = width // 4
    piece = width // PIECES

    def expert_rows(offsets):
        slabs = [slab_of(o) for o in offsets]
        lhs = jnp.concatenate([rows[w, k, :, :width] for w in slabs for k in range(2)], axis=0)
        tail = jnp.concatenate([rows[w, k, :, width:] for w in slabs for k in range(2)], axis=0)
        lanes = lax.broadcasted_iota(jnp.int32, tail.shape, 1)
        chosen = (lanes == mine_expert) | (lanes == mine_expert + EXPERTS)
        weight = jnp.sum(jnp.where(chosen, tail.astype(F32), 0.0), axis=-1, keepdims=True)
        gate = lax.dot_general(lhs, wg[...], nt, preferred_element_type=F32)
        up = lax.dot_general(lhs, wu[...], nt, preferred_element_type=F32)
        act = (jax.nn.silu(gate) * up * weight).astype(BF16)
        for c in range(4):
            cut = slice(c * quarter, (c + 1) * quarter)
            value = jnp.dot(act, wd[:, cut], preferred_element_type=F32)
            for i, w in enumerate(slabs):
                base = 2 * i * class_rows
                mine[w, :, cut] = value[base : base + class_rows]
                pair_out[w, :, cut] = value[base + class_rows : base + 2 * class_rows].astype(BF16)

    def pair_copy(way, d):
        slab = slab_of(-d if way == 0 else d)
        return remote(
            pair_out.at[slab], pair_in.at[slab], pr_send.at[0], pr_recv.at[d], partner
        )

    def pair_wait(d, count):
        whole(pair_in.at[pl.ds(0, count)], pr_send.at[0], pr_recv.at[d]).wait_recv()

    def next_rows(d):
        d2_wait(d, 2)
        expert_rows([d, -d])
        pair_copy(0, d).start()
        pair_copy(1, d).start()

    lax.fori_loop(1, half - 1, gather_step, 0)
    for p in range(PIECES):
        for way, sign in sides:
            ag_copy(way, sign, half - 2, p).wait_recv()
            if p in last_pieces(way):
                ag_copy(way, sign, half - 1, p, 1).start()
    for way, sign in sides:
        d2_copy(way, sign, half - 1).start()
    for copy in w_copies:
        copy.wait()
    next_rows(half - 2)
    for way, sign in sides:
        for p in last_pieces(way):
            ag_copy(way, sign, half - 1, p).wait_recv()
    d2_copy(0, -1, half).start()
    next_rows(half - 1)
    d2_wait(half, 1)
    expert_rows([half])
    pair_copy(0, half).start()

    def rs_copy(way, d, p, last=0):
        cut = pl.ds(p * piece, piece)
        return remote(
            ring_out.at[way, d - 1, :, cut], ring_in.at[way, d - 1, :, cut],
            rs_send.at[way, last], rs_recv.at[way, d - 1, p], step_to[way],
        )

    def local_sum(slab, p):
        cut = slice(p * piece, (p + 1) * piece)
        return mine[slab, :, cut] + pair_in[slab, :, cut].astype(F32)

    def pass_on(d, has_input):
        for p in range(PIECES):
            for way in range(2):
                cut = slice(p * piece, (p + 1) * piece)
                total = local_sum(slab_of(d if way == 0 else -d), p)
                if has_input(way, p):
                    rs_copy(way, d + 1, p).wait_recv()
                    total = total + ring_in[way, d, :, cut].astype(F32)
                ring_out[way, d - 1, :, cut] = total.astype(BF16)
                rs_copy(way, d, p).start()

    pair_wait(half, 1)
    for way in range(2):
        for p in last_pieces(way):
            cut = slice(p * piece, (p + 1) * piece)
            ring_out[way, half - 1, :, cut] = local_sum(slab_of(half), p).astype(BF16)
            rs_copy(way, half, p, 1).start()
    pair_wait(half - 1, 2)
    next_rows(half - 3)
    pass_on(half - 1, lambda way, p: p in last_pieces(way))

    def sum_step(i, carry):
        d = half - 2 - i
        next_rows(d - 2)
        pair_wait(d, 2)
        pass_on(d, lambda way, p: True)
        return carry

    lax.fori_loop(0, half - 4, sum_step, 0)
    d2_wait(0, 1)
    expert_rows([0])
    pair_copy(0, 0).start()
    for d in (2, 1):
        pair_wait(d, 2)
        pass_on(d, lambda way, p: True)

    pair_wait(0, 1)
    for p in range(PIECES):
        cut = slice(p * piece, (p + 1) * piece)
        total = local_sum(z, p)
        for way in range(2):
            rs_copy(way, 1, p).wait_recv()
            total = total + ring_in[way, 0, :, cut].astype(F32)
        for j in range(XS):
            xs_out[j, :, cut] = total[j * ROWS : (j + 1) * ROWS].astype(BF16)
    for k, p in enumerate(x_peers):
        remote(xs_out.at[p], xs_in.at[k], xs_send.at[0], xs_recv.at[0], at(z, p, core)).start()
    result = carried_ref[...] + xs_out[x].astype(F32)
    xs_all = whole(xs_in, xs_send.at[0], xs_recv.at[0])
    xs_all.wait_recv()
    for k in range(XS - 1):
        result = result + xs_in[k].astype(F32)
    for d in range(DOC_DEV):
        for t in range(NEW):
            r = d * NEW + t
            out_ref[t, d : d + 1, :] = result[r : r + 1].astype(BF16)

    xg_all.wait_send()
    xs_all.wait_send()
    for way in range(2):
        part = pl.ds(cuts[last_pieces(way)[0]], cuts[last_pieces(way)[-1] + 1] - cuts[last_pieces(way)[0]])
        whole(rows.at[pl.ds(0, half - 1), 0], ag_send.at[way, 0], ag_recv.at[0, 0, 0]).wait_send()
        whole(rows.at[0, 0, :, part], ag_send.at[way, 1], ag_recv.at[0, 0, 0]).wait_send()
        whole(ring_out.at[0, pl.ds(0, half - 1)], rs_send.at[way, 0], rs_recv.at[0, 0, 0]).wait_send()
        whole(
            ring_out.at[0, 0, :, pl.ds(0, width // 2)], rs_send.at[way, 1], rs_recv.at[0, 0, 0]
        ).wait_send()
    whole(rows.at[:, 0], d2_send.at[0], d2_recv.at[0]).wait_send()
    whole(pair_out, pr_send.at[0], pr_recv.at[0]).wait_send()


def per_device(
    hidden_in, norm_gain, queries, new_keys, new_values, cache_keys, cache_values,
    lengths, routes, gate_logits, w_gate, w_up, w_down,
):
    nz = lax.axis_size("dp") // (XS * CORES)
    half = nz // 2
    width = hidden_in.shape[2]
    docs, cache_len, kv_width = cache_keys.shape
    hidden = w_gate.shape[0]
    full = width + EXT
    class_rows = XS * ROWS
    vmem = pl.BlockSpec(memory_space=pltpu.VMEM)
    smem = pl.BlockSpec(memory_space=pltpu.SMEM)
    hbm = pl.BlockSpec(memory_space=pl.ANY)
    dma = pltpu.SemaphoreType.DMA
    return pl.pallas_call(
        functools.partial(layer_kernel, nz),
        name="layer",
        out_shape=jax.ShapeDtypeStruct(hidden_in.shape, BF16),
        in_specs=[hbm] * 7 + [smem] * 3 + [hbm] * 3,
        out_specs=vmem,
        scratch_shapes=[
            pltpu.VMEM(hidden_in.shape, BF16),
            pltpu.VMEM((1, width), F32),
            pltpu.VMEM(queries.shape, BF16),
            pltpu.VMEM(new_keys.shape, BF16),
            pltpu.VMEM(new_values.shape, BF16),
            pltpu.VMEM((docs, cache_len + TAIL, kv_width), BF16),
            pltpu.VMEM((docs, cache_len + TAIL, kv_width), BF16),
            pltpu.VMEM((hidden, width), BF16),
            pltpu.VMEM((hidden, width), BF16),
            pltpu.VMEM((hidden, width), BF16),
            pltpu.VMEM((ROWS, width), F32),
            pltpu.VMEM((XS, ROWS, full), BF16),
            pltpu.VMEM((nz, 2, class_rows, full), BF16),
            pltpu.VMEM((nz, class_rows, width), F32),
            pltpu.VMEM((nz, class_rows, width), BF16),
            pltpu.VMEM((nz, class_rows, width), BF16),
            pltpu.VMEM((2, half, class_rows, width), BF16),
            pltpu.VMEM((2, half, class_rows, width), BF16),
            pltpu.VMEM((XS, ROWS, width), BF16),
            pltpu.VMEM((XS - 1, ROWS, width), BF16),
            dma((5,)), dma((docs, 2)), dma((3,)),
            dma((1,)), dma((1,)),
            dma((2, 2)), dma((2, half, PIECES)),
            dma((1,)), dma((half + 1,)),
            dma((1,)), dma((half + 1,)),
            dma((2, 2)), dma((2, half, PIECES)),
            dma((1,)), dma((1,)),
        ],
        compiler_params=pltpu.CompilerParams(
            collective_id=0, has_side_effects=True, vmem_limit_bytes=56 * 1024 * 1024
        ),
    )(
        hidden_in, norm_gain.reshape(1, width), queries, new_keys, new_values, cache_keys,
        cache_values, lengths, routes, gate_logits, w_gate, w_up, w_down,
    )


def solution(mesh):
    in_specs = (
        P(None, ("grp", "dp"), None),
        P(),
        P(None, ("grp", "dp"), None),
        P(None, ("grp", "dp"), None),
        P(None, ("grp", "dp"), None),
        P(("grp", "dp"), None, None),
        P(("grp", "dp"), None, None),
        P(("grp", "dp")),
        P(None, ("grp", "dp"), None),
        P(None, ("grp", "dp"), None),
        P("dp", None),
        P("dp", None),
        P("dp", None),
    )
    out_specs = P(None, ("grp", "dp"), None)
    return jax.shard_map(
        per_device, mesh=mesh, in_specs=in_specs, out_specs=out_specs, check_vma=False
    )
```

```python
import functools

import jax
import jax.numpy as jnp
from jax import lax
from jax.experimental import pallas as pl
from jax.experimental.pallas import tpu as pltpu
from jax.sharding import PartitionSpec as P

HEADS = 32
KV_HEADS = 8
HEAD_DIM = 128
EXPERTS = 4
NEW = 2
DOC_DEV = 2
ROWS = NEW * DOC_DEV
EXT = 128
TAIL = 128
XS = 4
RADIUS = 2
PIECES = 4
CORES = 2
MESH = pl.DeviceIdType.MESH
F32 = jnp.float32
BF16 = jnp.bfloat16


def layer_kernel(
    nz, hid_hbm, gain_hbm, q_hbm, nk_hbm, nv_hbm, ck_hbm, cv_hbm, len_ref, routes_ref, logits_ref,
    wg_hbm, wu_hbm, wd_hbm, out_ref,
    hid, gain, q, nk, nv, kbuf, vbuf, wg, wu, wd, carried_ref,
    cols, rows, mine, pair_out, pair_in, ring_out, ring_in, xs_out, xs_in,
    in_sems, kv_sems, w_sems, zg_send, zg_recv, xf_send, xf_recv, xr_send, xr_recv, d2_send, d2_recv,
    pr_send, pr_recv, rs_send, rs_recv, xs_send, xs_recv,
):
    me = lax.axis_index("dp")
    core = me % CORES
    x = (me // CORES) % XS
    z = me // (CORES * XS)
    half = nz // 2
    width = carried_ref.shape[1]
    full = width + EXT
    class_rows = XS * ROWS
    mine_expert = z // (nz // EXPERTS)
    docs, span, kv_width = kbuf.shape
    cache_len = span - TAIL

    def at(zz, xx, cc):
        return {"dp": (zz * XS + xx) * CORES + cc}

    def slab_of(offset):
        return lax.rem(z + offset + nz, nz)

    partner = at(z, x, 1 - core)
    step_to = (at(slab_of(1), x, core), at(slab_of(-1), x, core))
    x_peers = [lax.rem(x + k, XS) for k in range(1, XS)]

    barrier = pltpu.get_barrier_semaphore()
    greeted = [partner] + [at(z, p, core) for p in x_peers]
    for r in range(1, RADIUS + 1):
        greeted += [at(slab_of(r), x, core), at(slab_of(-r), x, core)]
    for device in greeted:
        pl.semaphore_signal(barrier, inc=1, device_id=device, device_id_type=MESH)

    small = [
        pltpu.make_async_copy(src, dst, in_sems.at[i])
        for i, (src, dst) in enumerate(
            ((q_hbm, q), (nk_hbm, nk), (nv_hbm, nv), (hid_hbm, hid), (gain_hbm, gain))
        )
    ]
    kv = [
        pltpu.make_async_copy(src.at[d], dst.at[d, pl.ds(0, cache_len)], kv_sems.at[d, i])
        for d in range(docs)
        for i, (src, dst) in enumerate(((ck_hbm, kbuf), (cv_hbm, vbuf)))
    ]
    w_copies = [
        pltpu.make_async_copy(src, dst, w_sems.at[i])
        for i, (src, dst) in enumerate(((wg_hbm, wg), (wu_hbm, wu), (wd_hbm, wd)))
    ]
    for copy in small[:3] + kv + small[3:] + w_copies:
        copy.start()

    heads_rows = HEADS * NEW
    per_kv = heads_rows // KV_HEADS
    col = lax.broadcasted_iota(jnp.int32, (heads_rows, span), 1)
    row_at = lax.broadcasted_iota(jnp.int32, (heads_rows, span), 0)
    fresh_ok = (col == cache_len) | ((col == cache_len + 1) & (row_at % NEW == 1))
    block = (
        lax.broadcasted_iota(jnp.int32, (heads_rows, kv_width), 0) // per_kv
        == lax.broadcasted_iota(jnp.int32, (heads_rows, kv_width), 1) // HEAD_DIM
    )
    zeros = jnp.zeros((TAIL - NEW, kv_width), F32)

    lane = lax.broadcasted_iota(jnp.int32, (ROWS, EXT), 1)
    at_row = lax.broadcasted_iota(jnp.int32, (ROWS, EXT), 0)

    def by_row(values):
        out = jnp.full((ROWS, EXT), values[0])
        for r in range(1, ROWS):
            out = jnp.where(at_row == r, values[r], out)
        return out

    order = [(t, d) for d in range(DOC_DEV) for t in range(NEW)]
    first = by_row([routes_ref[t, d, 0] for t, d in order])
    second = by_row([routes_ref[t, d, 1] for t, d in order])
    share = jax.nn.sigmoid(by_row([logits_ref[t, d, 0] - logits_ref[t, d, 1] for t, d in order]))
    expert_at = lane % EXPERTS
    weights = jnp.where(expert_at == first, share, 0.0) + jnp.where(
        expert_at == second, 1.0 - share, 0.0
    )
    high = weights.astype(BF16)
    low = (weights - high.astype(F32)).astype(BF16)
    zero_ext = jnp.zeros_like(high)
    ext = jnp.where(lane < EXPERTS, high, jnp.where(lane < 2 * EXPERTS, low, zero_ext))

    for copy in small[:3]:
        copy.wait()
    q_all = q[...].astype(F32)
    nk_all = nk[...].astype(F32)
    nv_all = nv[...].astype(F32)
    q_blocks = []
    for d in range(docs):
        kbuf[d, cache_len:, :] = jnp.concatenate([nk_all[:, d, :], zeros], axis=0).astype(BF16)
        vbuf[d, cache_len:, :] = jnp.concatenate([nv_all[:, d, :], zeros], axis=0).astype(BF16)
        q_doc = q_all[:, d, :]
        q_rows = jnp.concatenate(
            [q_doc[:, h * HEAD_DIM : (h + 1) * HEAD_DIM] for h in range(HEADS)], axis=0
        )
        q_blocks.append(
            jnp.where(block, jnp.concatenate([q_rows] * KV_HEADS, axis=1), 0.0).astype(BF16)
        )
    parts = []
    for d in range(docs):
        kv[2 * d].wait()
        scores = lax.dot_general(
            q_blocks[d], kbuf[d], (((1,), (1,)), ((), ())), preferred_element_type=F32
        ) * (HEAD_DIM ** (-0.5))
        keep = (col < len_ref[d]) | fresh_ok
        scores = jnp.where(keep, scores, -1e30)
        e = jnp.exp(scores - jnp.max(scores, -1, keepdims=True))
        probs = (e / jnp.sum(e, -1, keepdims=True)).astype(BF16)
        kv[2 * d + 1].wait()
        out = jnp.dot(probs, vbuf[d], preferred_element_type=F32)
        pieces = []
        for h in range(HEADS):
            k = h * NEW // per_kv
            pieces.append(out[h * NEW : (h + 1) * NEW, k * HEAD_DIM : (k + 1) * HEAD_DIM])
        parts.append(jnp.concatenate(pieces, axis=1))
    for copy in small[3:]:
        copy.wait()
    hid_all = hid[...].astype(F32)
    carried = jnp.concatenate([hid_all[:, d, :] + parts[d] for d in range(docs)], axis=0)
    carried_ref[...] = carried
    normed = carried * lax.rsqrt(jnp.mean(carried * carried, -1, keepdims=True) + 1e-05)
    cols[z, x, :, :width] = (normed * gain[...]).astype(BF16)
    cols[z, x, :, width:] = ext
    pl.semaphore_wait(barrier, len(greeted))

    def remote(src, dst, send, recv, device):
        return pltpu.make_async_remote_copy(
            src_ref=src, dst_ref=dst, send_sem=send, recv_sem=recv,
            device_id=device, device_id_type=MESH,
        )

    def whole(ref, send, recv):
        return remote(ref, ref, send, recv, partner)

    sides = ((0, -1), (1, 1))
    x_to = (at(z, lax.rem(x + 1, XS), core), at(z, lax.rem(x + XS - 1, XS), core))
    x_from = (lax.rem(x + XS - 1, XS), lax.rem(x + 1, XS))
    middle = full // 256 * 128
    halves = (pl.ds(0, middle), pl.ds(middle, full - middle))

    def zg_copy(way, sign, leg, r):
        d = leg * RADIUS + r
        ref = cols.at[slab_of(sign * leg * RADIUS), x]
        if d == half:
            ref = ref.at[:, halves[way]]
        to = at(slab_of(-sign * r), x, core)
        return remote(ref, ref, zg_send.at[way, int(d == half)], zg_recv.at[way, d - 1], to)

    def send_leg(leg, way, sign):
        for r in range(RADIUS, 0, -1):
            zg_copy(way, sign, leg, r).start()

    def ways_of(d):
        return sides[:1] if d in (0, half) else sides

    def spread(d):
        for way, sign in ways_of(d):
            for side in range(2):
                ref = cols.at[slab_of(sign * d), x]
                remote(ref, ref, xf_send.at[0], xf_recv.at[d, side], x_to[side]).start()

    def relay(d):
        for side in range(2):
            count = len(ways_of(d))
            whole(cols.at[pl.ds(0, count), 0], xf_send.at[0], xf_recv.at[d, side]).wait_recv()
            for way, sign in ways_of(d):
                ref = cols.at[slab_of(sign * d), x_from[side], :, halves[side]]
                remote(ref, ref, xr_send.at[0], xr_recv.at[d], x_to[side]).start()

    def collect(d):
        count = len(ways_of(d))
        whole(cols.at[pl.ds(0, count), 0], xr_send.at[0], xr_recv.at[d]).wait_recv()
        for way, sign in ways_of(d):
            slab = slab_of(sign * d)
            rows[slab, 0] = jnp.concatenate(
                [cols[slab, j].astype(F32) for j in range(XS)], axis=0
            ).astype(BF16)
            d2_copy(way, sign, d).start()

    def d2_copy(way, sign, s):
        slab = slab_of(sign * s)
        return remote(rows.at[slab, 0], rows.at[slab, 1], d2_send.at[0], d2_recv.at[s], partner)

    def d2_wait(s, count):
        whole(rows.at[pl.ds(0, count), 1], d2_send.at[0], d2_recv.at[s]).wait_recv()

    def last_pieces(way):
        return tuple(range(PIECES // 2)) if way == 0 else tuple(range(PIECES // 2, PIECES))

    nt = (((1,), (1,)), ((), ()))
    quarter = width // 4
    piece = width // PIECES

    def expert_rows(offsets):
        slabs = [slab_of(o) for o in offsets]
        lhs = jnp.concatenate([rows[w, k, :, :width] for w in slabs for k in range(2)], axis=0)
        tail = jnp.concatenate([rows[w, k, :, width:] for w in slabs for k in range(2)], axis=0)
        lanes = lax.broadcasted_iota(jnp.int32, tail.shape, 1)
        chosen = (lanes == mine_expert) | (lanes == mine_expert + EXPERTS)
        weight = jnp.sum(jnp.where(chosen, tail.astype(F32), 0.0), axis=-1, keepdims=True)
        gate = lax.dot_general(lhs, wg[...], nt, preferred_element_type=F32)
        up = lax.dot_general(lhs, wu[...], nt, preferred_element_type=F32)
        act = (jax.nn.silu(gate) * up * weight).astype(BF16)
        for c in range(4):
            cut = slice(c * quarter, (c + 1) * quarter)
            value = jnp.dot(act, wd[:, cut], preferred_element_type=F32)
            for i, w in enumerate(slabs):
                base = 2 * i * class_rows
                mine[w, :, cut] = value[base : base + class_rows]
                pair_out[w, :, cut] = value[base + class_rows : base + 2 * class_rows].astype(BF16)

    def pair_copy(way, d):
        slab = slab_of(-d if way == 0 else d)
        return remote(
            pair_out.at[slab], pair_in.at[slab], pr_send.at[0], pr_recv.at[d], partner
        )

    def pair_wait(d, count):
        whole(pair_in.at[pl.ds(0, count)], pr_send.at[0], pr_recv.at[d]).wait_recv()

    def next_rows(d):
        d2_wait(d, 2)
        expert_rows([d, -d])
        pair_copy(0, d).start()
        pair_copy(1, d).start()

    for way, sign in sides:
        send_leg(0, way, sign)
    spread(0)
    relay(0)
    legs = half // RADIUS
    waiting = [0]
    for leg in range(legs):
        near = leg * RADIUS
        landed = [near + r for r in range(RADIUS, 0, -1)]
        for d in landed:
            for way, sign in sides:
                zg_copy(way, sign, leg, d - near).wait_recv()
                if d == near + RADIUS and leg < legs - 1:
                    send_leg(leg + 1, way, sign)
            spread(d)
        for d in waiting:
            collect(d)
        for d in landed:
            relay(d)
        waiting = landed
    for copy in w_copies:
        copy.wait()
    next_rows(half - 2)
    for d in waiting:
        collect(d)
    next_rows(half - 3)
    d2_wait(half, 1)
    expert_rows([half])
    pair_copy(0, half).start()
    next_rows(half - 1)

    def rs_copy(way, d, p, last=0):
        cut = pl.ds(p * piece, piece)
        return remote(
            ring_out.at[way, d - 1, :, cut], ring_in.at[way, d - 1, :, cut],
            rs_send.at[way, last], rs_recv.at[way, d - 1, p], step_to[way],
        )

    def local_sum(slab, p):
        cut = slice(p * piece, (p + 1) * piece)
        return mine[slab, :, cut] + pair_in[slab, :, cut].astype(F32)

    def pass_on(d, has_input):
        for p in range(PIECES):
            for way in range(2):
                cut = slice(p * piece, (p + 1) * piece)
                total = local_sum(slab_of(d if way == 0 else -d), p)
                if has_input(way, p):
                    rs_copy(way, d + 1, p).wait_recv()
                    total = total + ring_in[way, d, :, cut].astype(F32)
                ring_out[way, d - 1, :, cut] = total.astype(BF16)
                rs_copy(way, d, p).start()

    pair_wait(half, 1)
    for way in range(2):
        for p in last_pieces(way):
            cut = slice(p * piece, (p + 1) * piece)
            ring_out[way, half - 1, :, cut] = local_sum(slab_of(half), p).astype(BF16)
            rs_copy(way, half, p, 1).start()
    pair_wait(half - 1, 2)
    pass_on(half - 1, lambda way, p: p in last_pieces(way))

    def sum_step(i, carry):
        d = half - 2 - i
        next_rows(d - 2)
        pair_wait(d, 2)
        pass_on(d, lambda way, p: True)
        return carry

    lax.fori_loop(0, half - 4, sum_step, 0)
    d2_wait(0, 1)
    expert_rows([0])
    pair_copy(0, 0).start()
    for d in (2, 1):
        pair_wait(d, 2)
        pass_on(d, lambda way, p: True)

    pair_wait(0, 1)
    for p in range(PIECES):
        cut = slice(p * piece, (p + 1) * piece)
        total = local_sum(z, p)
        for way in range(2):
            rs_copy(way, 1, p).wait_recv()
            total = total + ring_in[way, 0, :, cut].astype(F32)
        for j in range(XS):
            xs_out[j, :, cut] = total[j * ROWS : (j + 1) * ROWS].astype(BF16)
    for k, p in enumerate(x_peers):
        remote(xs_out.at[p], xs_in.at[k], xs_send.at[0], xs_recv.at[0], at(z, p, core)).start()
    result = carried_ref[...] + xs_out[x].astype(F32)
    xs_all = whole(xs_in, xs_send.at[0], xs_recv.at[0])
    xs_all.wait_recv()
    for k in range(XS - 1):
        result = result + xs_in[k].astype(F32)
    for d in range(DOC_DEV):
        for t in range(NEW):
            r = d * NEW + t
            out_ref[t, d : d + 1, :] = result[r : r + 1].astype(BF16)

    xs_all.wait_send()
    whole(cols.at[:, pl.ds(0, 2)], xf_send.at[0], xf_recv.at[0, 0]).wait_send()
    whole(cols.at[:, 0], xr_send.at[0], xr_recv.at[0]).wait_send()
    for way in range(2):
        whole(cols.at[pl.ds(0, half - 1), 0], zg_send.at[way, 0], zg_recv.at[0, 0]).wait_send()
        whole(cols.at[0, 0, :, halves[way]], zg_send.at[way, 1], zg_recv.at[0, 0]).wait_send()
        whole(ring_out.at[0, pl.ds(0, half - 1)], rs_send.at[way, 0], rs_recv.at[0, 0, 0]).wait_send()
        whole(
            ring_out.at[0, 0, :, pl.ds(0, width // 2)], rs_send.at[way, 1], rs_recv.at[0, 0, 0]
        ).wait_send()
    whole(rows.at[:, 0], d2_send.at[0], d2_recv.at[0]).wait_send()
    whole(pair_out, pr_send.at[0], pr_recv.at[0]).wait_send()


def per_device(
    hidden_in, norm_gain, queries, new_keys, new_values, cache_keys, cache_values,
    lengths, routes, gate_logits, w_gate, w_up, w_down,
):
    nz = lax.axis_size("dp") // (XS * CORES)
    half = nz // 2
    width = hidden_in.shape[2]
    docs, cache_len, kv_width = cache_keys.shape
    hidden = w_gate.shape[0]
    full = width + EXT
    class_rows = XS * ROWS
    vmem = pl.BlockSpec(memory_space=pltpu.VMEM)
    smem = pl.BlockSpec(memory_space=pltpu.SMEM)
    hbm = pl.BlockSpec(memory_space=pl.ANY)
    dma = pltpu.SemaphoreType.DMA
    return pl.pallas_call(
        functools.partial(layer_kernel, nz),
        name="layer",
        out_shape=jax.ShapeDtypeStruct(hidden_in.shape, BF16),
        in_specs=[hbm] * 7 + [smem] * 3 + [hbm] * 3,
        out_specs=vmem,
        scratch_shapes=[
            pltpu.VMEM(hidden_in.shape, BF16),
            pltpu.VMEM((1, width), F32),
            pltpu.VMEM(queries.shape, BF16),
            pltpu.VMEM(new_keys.shape, BF16),
            pltpu.VMEM(new_values.shape, BF16),
            pltpu.VMEM((docs, cache_len + TAIL, kv_width), BF16),
            pltpu.VMEM((docs, cache_len + TAIL, kv_width), BF16),
            pltpu.VMEM((hidden, width), BF16),
            pltpu.VMEM((hidden, width), BF16),
            pltpu.VMEM((hidden, width), BF16),
            pltpu.VMEM((ROWS, width), F32),
            pltpu.VMEM((nz, XS, ROWS, full), BF16),
            pltpu.VMEM((nz, 2, class_rows, full), BF16),
            pltpu.VMEM((nz, class_rows, width), F32),
            pltpu.VMEM((nz, class_rows, width), BF16),
            pltpu.VMEM((nz, class_rows, width), BF16),
            pltpu.VMEM((2, half, class_rows, width), BF16),
            pltpu.VMEM((2, half, class_rows, width), BF16),
            pltpu.VMEM((XS, ROWS, width), BF16),
            pltpu.VMEM((XS - 1, ROWS, width), BF16),
            dma((5,)), dma((docs, 2)), dma((3,)),
            dma((2, 2)), dma((2, half)),
            dma((1,)), dma((half + 1, 2)),
            dma((1,)), dma((half + 1,)),
            dma((1,)), dma((half + 1,)),
            dma((1,)), dma((half + 1,)),
            dma((2, 2)), dma((2, half, PIECES)),
            dma((1,)), dma((1,)),
        ],
        compiler_params=pltpu.CompilerParams(
            collective_id=0, has_side_effects=True, vmem_limit_bytes=56 * 1024 * 1024
        ),
    )(
        hidden_in, norm_gain.reshape(1, width), queries, new_keys, new_values, cache_keys,
        cache_values, lengths, routes, gate_logits, w_gate, w_up, w_down,
    )


def solution(mesh):
    in_specs = (
        P(None, ("grp", "dp"), None),
        P(),
        P(None, ("grp", "dp"), None),
        P(None, ("grp", "dp"), None),
        P(None, ("grp", "dp"), None),
        P(("grp", "dp"), None, None),
        P(("grp", "dp"), None, None),
        P(("grp", "dp")),
        P(None, ("grp", "dp"), None),
        P(None, ("grp", "dp"), None),
        P("dp", None),
        P("dp", None),
        P("dp", None),
    )
    out_specs = P(None, ("grp", "dp"), None)
    return jax.shard_map(
        per_device, mesh=mesh, in_specs=in_specs, out_specs=out_specs, check_vma=False
    )
```

```python
import functools

import jax
import jax.numpy as jnp
from jax import lax
from jax.experimental import pallas as pl
from jax.experimental.pallas import tpu as pltpu
from jax.sharding import PartitionSpec as P

HEADS = 32
KV_HEADS = 8
HEAD_DIM = 128
EXPERTS = 4
NEW = 2
DOC_DEV = 2
ROWS = NEW * DOC_DEV
EXT = 128
TAIL = 128
XS = 4
RADIUS = 2
CORES = 2
MESH = pl.DeviceIdType.MESH
F32 = jnp.float32
BF16 = jnp.bfloat16


def layer_kernel(
    nz, hid_hbm, gain_hbm, q_hbm, nk_hbm, nv_hbm, ck_hbm, cv_hbm, len_ref, routes_ref, logits_ref,
    wg_hbm, wu_hbm, wd_hbm, out_ref,
    hid, gain, q, nk, nv, kbuf, vbuf, wg, wu, wd, carried_ref,
    cols, rows, mine, pair_out, pair_in, quad, far_out, far_in, near_out, near_in, z_out, z_in,
    in_sems, kv_sems, w_sems, zg_send, zg_recv, xf_send, xf_recv, xr_send, xr_recv, d2_send, d2_recv,
    pr_send, pr_recv, far_send, far_recv, near_send, near_recv, zs_send, zs_recv,
):
    me = lax.axis_index("dp")
    core = me % CORES
    x = (me // CORES) % XS
    z = me // (CORES * XS)
    half = nz // 2
    width = carried_ref.shape[1]
    full = width + EXT
    class_rows = XS * ROWS
    mine_expert = z // (nz // EXPERTS)
    docs, span, kv_width = kbuf.shape
    cache_len = span - TAIL

    def at(zz, xx, cc):
        return {"dp": (zz * XS + xx) * CORES + cc}

    def slab_of(offset):
        return lax.rem(z + offset + nz, nz)

    partner = at(z, x, 1 - core)
    x_next = (lax.rem(x + 1, XS), lax.rem(x + XS - 1, XS))
    x_far = lax.rem(x + 2, XS)

    barrier = pltpu.get_barrier_semaphore()
    greeted = [partner] + [at(z, p, core) for p in x_next]
    for r in range(1, RADIUS + 1):
        greeted += [at(slab_of(r), x, core), at(slab_of(-r), x, core)]
    for device in greeted:
        pl.semaphore_signal(barrier, inc=1, device_id=device, device_id_type=MESH)

    small = [
        pltpu.make_async_copy(src, dst, in_sems.at[i])
        for i, (src, dst) in enumerate(
            ((q_hbm, q), (nk_hbm, nk), (nv_hbm, nv), (hid_hbm, hid), (gain_hbm, gain))
        )
    ]
    kv = [
        pltpu.make_async_copy(src.at[d], dst.at[d, pl.ds(0, cache_len)], kv_sems.at[d, i])
        for d in range(docs)
        for i, (src, dst) in enumerate(((ck_hbm, kbuf), (cv_hbm, vbuf)))
    ]
    w_copies = [
        pltpu.make_async_copy(src, dst, w_sems.at[i])
        for i, (src, dst) in enumerate(((wg_hbm, wg), (wu_hbm, wu), (wd_hbm, wd)))
    ]
    for copy in small[:3] + kv + small[3:] + w_copies:
        copy.start()

    heads_rows = HEADS * NEW
    per_kv = heads_rows // KV_HEADS
    col = lax.broadcasted_iota(jnp.int32, (heads_rows, span), 1)
    row_at = lax.broadcasted_iota(jnp.int32, (heads_rows, span), 0)
    fresh_ok = (col == cache_len) | ((col == cache_len + 1) & (row_at % NEW == 1))
    block = (
        lax.broadcasted_iota(jnp.int32, (heads_rows, kv_width), 0) // per_kv
        == lax.broadcasted_iota(jnp.int32, (heads_rows, kv_width), 1) // HEAD_DIM
    )
    zeros = jnp.zeros((TAIL - NEW, kv_width), F32)

    lane = lax.broadcasted_iota(jnp.int32, (ROWS, EXT), 1)
    at_row = lax.broadcasted_iota(jnp.int32, (ROWS, EXT), 0)

    def by_row(values):
        out = jnp.full((ROWS, EXT), values[0])
        for r in range(1, ROWS):
            out = jnp.where(at_row == r, values[r], out)
        return out

    order = [(t, d) for d in range(DOC_DEV) for t in range(NEW)]
    first = by_row([routes_ref[t, d, 0] for t, d in order])
    second = by_row([routes_ref[t, d, 1] for t, d in order])
    share = jax.nn.sigmoid(by_row([logits_ref[t, d, 0] - logits_ref[t, d, 1] for t, d in order]))
    expert_at = lane % EXPERTS
    weights = jnp.where(expert_at == first, share, 0.0) + jnp.where(
        expert_at == second, 1.0 - share, 0.0
    )
    high = weights.astype(BF16)
    low = (weights - high.astype(F32)).astype(BF16)
    zero_ext = jnp.zeros_like(high)
    ext = jnp.where(lane < EXPERTS, high, jnp.where(lane < 2 * EXPERTS, low, zero_ext))

    for copy in small[:3]:
        copy.wait()
    q_all = q[...].astype(F32)
    nk_all = nk[...].astype(F32)
    nv_all = nv[...].astype(F32)
    q_blocks = []
    for d in range(docs):
        kbuf[d, cache_len:, :] = jnp.concatenate([nk_all[:, d, :], zeros], axis=0).astype(BF16)
        vbuf[d, cache_len:, :] = jnp.concatenate([nv_all[:, d, :], zeros], axis=0).astype(BF16)
        q_doc = q_all[:, d, :]
        q_rows = jnp.concatenate(
            [q_doc[:, h * HEAD_DIM : (h + 1) * HEAD_DIM] for h in range(HEADS)], axis=0
        )
        q_blocks.append(
            jnp.where(block, jnp.concatenate([q_rows] * KV_HEADS, axis=1), 0.0).astype(BF16)
        )
    parts = []
    for d in range(docs):
        kv[2 * d].wait()
        scores = lax.dot_general(
            q_blocks[d], kbuf[d], (((1,), (1,)), ((), ())), preferred_element_type=F32
        ) * (HEAD_DIM ** (-0.5))
        keep = (col < len_ref[d]) | fresh_ok
        scores = jnp.where(keep, scores, -1e30)
        e = jnp.exp(scores - jnp.max(scores, -1, keepdims=True))
        probs = (e / jnp.sum(e, -1, keepdims=True)).astype(BF16)
        kv[2 * d + 1].wait()
        out = jnp.dot(probs, vbuf[d], preferred_element_type=F32)
        pieces = []
        for h in range(HEADS):
            k = h * NEW // per_kv
            pieces.append(out[h * NEW : (h + 1) * NEW, k * HEAD_DIM : (k + 1) * HEAD_DIM])
        parts.append(jnp.concatenate(pieces, axis=1))
    for copy in small[3:]:
        copy.wait()
    hid_all = hid[...].astype(F32)
    carried = jnp.concatenate([hid_all[:, d, :] + parts[d] for d in range(docs)], axis=0)
    carried_ref[...] = carried
    normed = carried * lax.rsqrt(jnp.mean(carried * carried, -1, keepdims=True) + 1e-05)
    cols[z, x, :, :width] = (normed * gain[...]).astype(BF16)
    cols[z, x, :, width:] = ext
    pl.semaphore_wait(barrier, len(greeted))

    def remote(src, dst, send, recv, device):
        return pltpu.make_async_remote_copy(
            src_ref=src, dst_ref=dst, send_sem=send, recv_sem=recv,
            device_id=device, device_id_type=MESH,
        )

    def whole(ref, send, recv):
        return remote(ref, ref, send, recv, partner)

    sides = ((0, -1), (1, 1))
    x_to = tuple(at(z, p, core) for p in x_next)
    x_from = x_next[::-1]
    middle = full // 256 * 128
    halves = (pl.ds(0, middle), pl.ds(middle, full - middle))

    def zg_copy(way, sign, leg, r):
        d = leg * RADIUS + r
        ref = cols.at[slab_of(sign * leg * RADIUS), x]
        if d == half:
            ref = ref.at[:, halves[way]]
        to = at(slab_of(-sign * r), x, core)
        return remote(ref, ref, zg_send.at[way, int(d == half)], zg_recv.at[way, d - 1], to)

    def send_leg(leg, way, sign):
        for r in range(RADIUS, 0, -1):
            zg_copy(way, sign, leg, r).start()

    def ways_of(d):
        return sides[:1] if d in (0, half) else sides

    def spread(d):
        for way, sign in ways_of(d):
            for side in range(2):
                ref = cols.at[slab_of(sign * d), x]
                remote(ref, ref, xf_send.at[0], xf_recv.at[d, side], x_to[side]).start()

    def relay(d):
        for side in range(2):
            count = len(ways_of(d))
            whole(cols.at[pl.ds(0, count), 0], xf_send.at[0], xf_recv.at[d, side]).wait_recv()
            for way, sign in ways_of(d):
                ref = cols.at[slab_of(sign * d), x_from[side], :, halves[side]]
                remote(ref, ref, xr_send.at[0], xr_recv.at[d], x_to[side]).start()

    def collect(d):
        count = len(ways_of(d))
        whole(cols.at[pl.ds(0, count), 0], xr_send.at[0], xr_recv.at[d]).wait_recv()
        for way, sign in ways_of(d):
            slab = slab_of(sign * d)
            rows[slab, 0] = jnp.concatenate(
                [cols[slab, j].astype(F32) for j in range(XS)], axis=0
            ).astype(BF16)
            d2_copy(way, sign, d).start()

    def d2_copy(way, sign, s):
        slab = slab_of(sign * s)
        return remote(rows.at[slab, 0], rows.at[slab, 1], d2_send.at[0], d2_recv.at[s], partner)

    def d2_wait(s, count):
        whole(rows.at[pl.ds(0, count), 1], d2_send.at[0], d2_recv.at[s]).wait_recv()

    nt = (((1,), (1,)), ((), ()))
    quarter = width // 4
    parts_of = (slice(0, width // 2), slice(width // 2, width))
    spans_of = (pl.ds(0, width // 2), pl.ds(width // 2, width // 2))

    def expert_rows(offsets):
        slabs = [slab_of(o) for o in offsets]
        lhs = jnp.concatenate([rows[w, k, :, :width] for w in slabs for k in range(2)], axis=0)
        tail = jnp.concatenate([rows[w, k, :, width:] for w in slabs for k in range(2)], axis=0)
        lanes = lax.broadcasted_iota(jnp.int32, tail.shape, 1)
        chosen = (lanes == mine_expert) | (lanes == mine_expert + EXPERTS)
        weight = jnp.sum(jnp.where(chosen, tail.astype(F32), 0.0), axis=-1, keepdims=True)
        gate = lax.dot_general(lhs, wg[...], nt, preferred_element_type=F32)
        up = lax.dot_general(lhs, wu[...], nt, preferred_element_type=F32)
        act = (jax.nn.silu(gate) * up * weight).astype(BF16)
        for c in range(4):
            cut = slice(c * quarter, (c + 1) * quarter)
            value = jnp.dot(act, wd[:, cut], preferred_element_type=F32)
            for i, w in enumerate(slabs):
                base = 2 * i * class_rows
                mine[w, :, cut] = value[base : base + class_rows]
                pair_out[w, :, cut] = value[base + class_rows : base + 2 * class_rows].astype(BF16)

    def pair_copy(way, d):
        slab = slab_of(-d if way == 0 else d)
        return remote(
            pair_out.at[slab], pair_in.at[slab], pr_send.at[0], pr_recv.at[d], partner
        )

    def pair_wait(d, count):
        whole(pair_in.at[pl.ds(0, count)], pr_send.at[0], pr_recv.at[d]).wait_recv()

    def next_rows(d):
        d2_wait(d, 2)
        expert_rows([d, -d])
        pair_copy(0, d).start()
        pair_copy(1, d).start()

    for way, sign in sides:
        send_leg(0, way, sign)
    spread(0)
    relay(0)
    legs = half // RADIUS
    waiting = [0]
    for leg in range(legs):
        near = leg * RADIUS
        landed = [near + r for r in range(RADIUS, 0, -1)]
        for d in landed:
            for way, sign in sides:
                zg_copy(way, sign, leg, d - near).wait_recv()
                if d == near + RADIUS and leg < legs - 1:
                    send_leg(leg + 1, way, sign)
            spread(d)
        for d in waiting:
            collect(d)
        for d in landed:
            relay(d)
        waiting = landed
    for copy in w_copies:
        copy.wait()
    next_rows(half - 2)
    for d in waiting:
        collect(d)
    next_rows(half - 3)

    def local_sum(d):
        pair_wait(d, len(ways_of(d)))
        for way, sign in ways_of(d):
            slab = slab_of(sign * d)
            total = mine[slab] + pair_in[slab].astype(F32)
            for j in range(XS):
                quad[slab, j] = total[j * ROWS : (j + 1) * ROWS]
            far_out[slab] = quad[slab, x_far].astype(BF16)
            for side in range(2):
                remote(
                    far_out.at[slab, :, spans_of[side]], far_in.at[slab, side],
                    far_send.at[0], far_recv.at[d], x_to[side],
                ).start()

    def neighbour_sum(d):
        count = len(ways_of(d))
        whole(far_out.at[pl.ds(0, count)], far_send.at[0], far_recv.at[d]).wait_recv()
        for way, sign in ways_of(d):
            slab = slab_of(sign * d)
            for side in range(2):
                col = x_next[side]
                here, there = parts_of[side], parts_of[1 - side]
                near_out[slab, side, :, here] = (
                    quad[slab, col, :, here] + far_in[slab, side].astype(F32)
                ).astype(BF16)
                near_out[slab, side, :, there] = quad[slab, col, :, there].astype(BF16)
                remote(
                    near_out.at[slab, side], near_in.at[slab, side],
                    near_send.at[0], near_recv.at[d], x_to[side],
                ).start()

    def zs_copy(way, sign, d):
        src, dst = z_out.at[way, d - 1], z_in.at[way, d - 1]
        if d == half:
            src, dst = src.at[:, spans_of[way]], dst.at[:, spans_of[way]]
        hop = d - (d - 1) // RADIUS * RADIUS
        to = at(slab_of(sign * hop), x, core)
        return remote(src, dst, zs_send.at[way, int(d == half)], zs_recv.at[way, d - 1], to)

    def column_sum(d):
        count = 2 * len(ways_of(d))
        whole(z_out.at[0, pl.ds(0, count)], near_send.at[0], near_recv.at[d]).wait_recv()
        for way, sign in ways_of(d):
            slab = slab_of(sign * d)
            taken = []
            if d % RADIUS == 0 and d < half:
                taken = [(w, s, d + r) for w, s in (sides if d == 0 else ((way, sign),)) for r in range(1, RADIUS + 1)]
            for w, s, e in taken:
                zs_copy(w, s, e).wait_recv()
            sums = []
            for h in range(2):
                cut = parts_of[h]
                total = quad[slab, x, :, cut]
                for side in range(2):
                    total = total + near_in[slab, side, :, cut].astype(F32)
                for w, s, e in taken:
                    if e < half or h == w:
                        total = total + z_in[w, e - 1, :, cut].astype(F32)
                sums.append(total)
            if d == 0:
                return jnp.concatenate(sums, axis=1)
            for w, s in sides if d == half else ((way, sign),):
                for h in range(2):
                    if d < half or h == w:
                        z_out[w, d - 1, :, parts_of[h]] = sums[h].astype(BF16)
                zs_copy(w, s, d).start()

    def last_rows(d):
        d2_wait(d, 1)
        expert_rows([d])
        pair_copy(0, d).start()

    last_rows(half)
    next_rows(half - 1)
    local_sum(half)
    next_rows(half - 4)
    local_sum(half - 1)
    neighbour_sum(half)
    local_sum(half - 2)
    next_rows(half - 5)
    neighbour_sum(half - 1)
    column_sum(half)
    local_sum(half - 3)
    next_rows(half - 6)
    neighbour_sum(half - 2)
    column_sum(half - 1)
    local_sum(half - 4)
    next_rows(half - 7)
    neighbour_sum(half - 3)
    local_sum(half - 5)
    last_rows(0)
    neighbour_sum(half - 4)
    column_sum(half - 3)
    local_sum(half - 6)
    neighbour_sum(half - 5)
    column_sum(half - 2)
    local_sum(half - 7)
    neighbour_sum(half - 6)
    column_sum(half - 5)
    local_sum(0)
    neighbour_sum(half - 7)
    column_sum(half - 4)
    neighbour_sum(0)
    column_sum(half - 7)
    column_sum(half - 6)
    result = carried_ref[...] + column_sum(0)
    for d in range(DOC_DEV):
        for t in range(NEW):
            r = d * NEW + t
            out_ref[t, d : d + 1, :] = result[r : r + 1].astype(BF16)

    whole(cols.at[:, pl.ds(0, 2)], xf_send.at[0], xf_recv.at[0, 0]).wait_send()
    whole(cols.at[:, 0], xr_send.at[0], xr_recv.at[0]).wait_send()
    for way in range(2):
        whole(cols.at[pl.ds(0, half - 1), 0], zg_send.at[way, 0], zg_recv.at[0, 0]).wait_send()
        whole(cols.at[0, 0, :, halves[way]], zg_send.at[way, 1], zg_recv.at[0, 0]).wait_send()
        whole(z_out.at[0, pl.ds(0, half - 1)], zs_send.at[way, 0], zs_recv.at[0, 0]).wait_send()
        whole(z_out.at[0, 0, :, spans_of[way]], zs_send.at[way, 1], zs_recv.at[0, 0]).wait_send()
    whole(far_out, far_send.at[0], far_recv.at[0]).wait_send()
    whole(near_out, near_send.at[0], near_recv.at[0]).wait_send()
    whole(rows.at[:, 0], d2_send.at[0], d2_recv.at[0]).wait_send()
    whole(pair_out, pr_send.at[0], pr_recv.at[0]).wait_send()


def per_device(
    hidden_in, norm_gain, queries, new_keys, new_values, cache_keys, cache_values,
    lengths, routes, gate_logits, w_gate, w_up, w_down,
):
    nz = lax.axis_size("dp") // (XS * CORES)
    half = nz // 2
    width = hidden_in.shape[2]
    docs, cache_len, kv_width = cache_keys.shape
    hidden = w_gate.shape[0]
    full = width + EXT
    class_rows = XS * ROWS
    vmem = pl.BlockSpec(memory_space=pltpu.VMEM)
    smem = pl.BlockSpec(memory_space=pltpu.SMEM)
    hbm = pl.BlockSpec(memory_space=pl.ANY)
    dma = pltpu.SemaphoreType.DMA
    return pl.pallas_call(
        functools.partial(layer_kernel, nz),
        name="layer",
        out_shape=jax.ShapeDtypeStruct(hidden_in.shape, BF16),
        in_specs=[hbm] * 7 + [smem] * 3 + [hbm] * 3,
        out_specs=vmem,
        scratch_shapes=[
            pltpu.VMEM(hidden_in.shape, BF16),
            pltpu.VMEM((1, width), F32),
            pltpu.VMEM(queries.shape, BF16),
            pltpu.VMEM(new_keys.shape, BF16),
            pltpu.VMEM(new_values.shape, BF16),
            pltpu.VMEM((docs, cache_len + TAIL, kv_width), BF16),
            pltpu.VMEM((docs, cache_len + TAIL, kv_width), BF16),
            pltpu.VMEM((hidden, width), BF16),
            pltpu.VMEM((hidden, width), BF16),
            pltpu.VMEM((hidden, width), BF16),
            pltpu.VMEM((ROWS, width), F32),
            pltpu.VMEM((nz, XS, ROWS, full), BF16),
            pltpu.VMEM((nz, 2, class_rows, full), BF16),
            pltpu.VMEM((nz, class_rows, width), F32),
            pltpu.VMEM((nz, class_rows, width), BF16),
            pltpu.VMEM((nz, class_rows, width), BF16),
            pltpu.VMEM((nz, XS, ROWS, width), F32),
            pltpu.VMEM((nz, ROWS, width), BF16),
            pltpu.VMEM((nz, 2, ROWS, width // 2), BF16),
            pltpu.VMEM((nz, 2, ROWS, width), BF16),
            pltpu.VMEM((nz, 2, ROWS, width), BF16),
            pltpu.VMEM((2, half, ROWS, width), BF16),
            pltpu.VMEM((2, half, ROWS, width), BF16),
            dma((5,)), dma((docs, 2)), dma((3,)),
            dma((2, 2)), dma((2, half)),
            dma((1,)), dma((half + 1, 2)),
            dma((1,)), dma((half + 1,)),
            dma((1,)), dma((half + 1,)),
            dma((1,)), dma((half + 1,)),
            dma((1,)), dma((half + 1,)),
            dma((1,)), dma((half + 1,)),
            dma((2, 2)), dma((2, half)),
        ],
        compiler_params=pltpu.CompilerParams(
            collective_id=0, has_side_effects=True, vmem_limit_bytes=56 * 1024 * 1024
        ),
    )(
        hidden_in, norm_gain.reshape(1, width), queries, new_keys, new_values, cache_keys,
        cache_values, lengths, routes, gate_logits, w_gate, w_up, w_down,
    )


def solution(mesh):
    in_specs = (
        P(None, ("grp", "dp"), None),
        P(),
        P(None, ("grp", "dp"), None),
        P(None, ("grp", "dp"), None),
        P(None, ("grp", "dp"), None),
        P(("grp", "dp"), None, None),
        P(("grp", "dp"), None, None),
        P(("grp", "dp")),
        P(None, ("grp", "dp"), None),
        P(None, ("grp", "dp"), None),
        P("dp", None),
        P("dp", None),
        P("dp", None),
    )
    out_specs = P(None, ("grp", "dp"), None)
    return jax.shard_map(
        per_device, mesh=mesh, in_specs=in_specs, out_specs=out_specs, check_vma=False
    )
```

```python
import functools

import jax
import jax.numpy as jnp
from jax import lax
from jax.experimental import pallas as pl
from jax.experimental.pallas import tpu as pltpu
from jax.sharding import PartitionSpec as P

HEADS = 32
KV_HEADS = 8
HEAD_DIM = 128
EXPERTS = 4
NEW = 2
DOC_DEV = 2
ROWS = NEW * DOC_DEV
EXT = 128
TAIL = 128
XS = 4
RADIUS = 2
BACK = 4
CORES = 2
MESH = pl.DeviceIdType.MESH
F32 = jnp.float32
BF16 = jnp.bfloat16


def layer_kernel(
    nz, hid_hbm, gain_hbm, q_hbm, nk_hbm, nv_hbm, ck_hbm, cv_hbm, len_ref, routes_ref, logits_ref,
    wg_hbm, wu_hbm, wd_hbm, out_ref,
    hid, gain, q, nk, nv, kbuf, vbuf, wg, wu, wd, carried_ref,
    cols, rows, mine, pair_out, pair_in, quad, far_out, far_in, near_out, near_in, z_out, z_in,
    in_sems, kv_sems, w_sems, zg_send, zg_recv, xf_send, xf_recv, xr_send, xr_recv, d2_send, d2_recv,
    pr_send, pr_recv, far_send, far_recv, near_send, near_recv, zs_send, zs_recv,
):
    me = lax.axis_index("dp")
    core = me % CORES
    x = (me // CORES) % XS
    z = me // (CORES * XS)
    half = nz // 2
    width = carried_ref.shape[1]
    full = width + EXT
    class_rows = XS * ROWS
    mine_expert = z // (nz // EXPERTS)
    docs, span, kv_width = kbuf.shape
    cache_len = span - TAIL

    def at(zz, xx, cc):
        return {"dp": (zz * XS + xx) * CORES + cc}

    def slab_of(offset):
        return lax.rem(z + offset + nz, nz)

    partner = at(z, x, 1 - core)
    x_next = (lax.rem(x + 1, XS), lax.rem(x + XS - 1, XS))
    x_far = lax.rem(x + 2, XS)

    barrier = pltpu.get_barrier_semaphore()
    greeted = [partner] + [at(z, p, core) for p in x_next]
    for r in range(1, max(RADIUS, BACK) + 1):
        greeted += [at(slab_of(r), x, core), at(slab_of(-r), x, core)]
    for device in greeted:
        pl.semaphore_signal(barrier, inc=1, device_id=device, device_id_type=MESH)

    small = [
        pltpu.make_async_copy(src, dst, in_sems.at[i])
        for i, (src, dst) in enumerate(
            ((q_hbm, q), (nk_hbm, nk), (nv_hbm, nv), (hid_hbm, hid), (gain_hbm, gain))
        )
    ]
    kv = [
        pltpu.make_async_copy(src.at[d], dst.at[d, pl.ds(0, cache_len)], kv_sems.at[d, i])
        for d in range(docs)
        for i, (src, dst) in enumerate(((ck_hbm, kbuf), (cv_hbm, vbuf)))
    ]
    w_copies = [
        pltpu.make_async_copy(src, dst, w_sems.at[i])
        for i, (src, dst) in enumerate(((wg_hbm, wg), (wu_hbm, wu), (wd_hbm, wd)))
    ]
    for copy in small[:3] + kv + small[3:] + w_copies:
        copy.start()

    heads_rows = HEADS * NEW
    per_kv = heads_rows // KV_HEADS
    col = lax.broadcasted_iota(jnp.int32, (heads_rows, span), 1)
    row_at = lax.broadcasted_iota(jnp.int32, (heads_rows, span), 0)
    fresh_ok = (col == cache_len) | ((col == cache_len + 1) & (row_at % NEW == 1))
    block = (
        lax.broadcasted_iota(jnp.int32, (heads_rows, kv_width), 0) // per_kv
        == lax.broadcasted_iota(jnp.int32, (heads_rows, kv_width), 1) // HEAD_DIM
    )
    zeros = jnp.zeros((TAIL - NEW, kv_width), F32)

    lane = lax.broadcasted_iota(jnp.int32, (ROWS, EXT), 1)
    at_row = lax.broadcasted_iota(jnp.int32, (ROWS, EXT), 0)

    def by_row(values):
        out = jnp.full((ROWS, EXT), values[0])
        for r in range(1, ROWS):
            out = jnp.where(at_row == r, values[r], out)
        return out

    order = [(t, d) for d in range(DOC_DEV) for t in range(NEW)]
    first = by_row([routes_ref[t, d, 0] for t, d in order])
    second = by_row([routes_ref[t, d, 1] for t, d in order])
    share = jax.nn.sigmoid(by_row([logits_ref[t, d, 0] - logits_ref[t, d, 1] for t, d in order]))
    expert_at = lane % EXPERTS
    weights = jnp.where(expert_at == first, share, 0.0) + jnp.where(
        expert_at == second, 1.0 - share, 0.0
    )
    high = weights.astype(BF16)
    low = (weights - high.astype(F32)).astype(BF16)
    zero_ext = jnp.zeros_like(high)
    ext = jnp.where(lane < EXPERTS, high, jnp.where(lane < 2 * EXPERTS, low, zero_ext))

    for copy in small[:3]:
        copy.wait()
    q_all = q[...].astype(F32)
    nk_all = nk[...].astype(F32)
    nv_all = nv[...].astype(F32)
    q_blocks = []
    for d in range(docs):
        kbuf[d, cache_len:, :] = jnp.concatenate([nk_all[:, d, :], zeros], axis=0).astype(BF16)
        vbuf[d, cache_len:, :] = jnp.concatenate([nv_all[:, d, :], zeros], axis=0).astype(BF16)
        q_doc = q_all[:, d, :]
        q_rows = jnp.concatenate(
            [q_doc[:, h * HEAD_DIM : (h + 1) * HEAD_DIM] for h in range(HEADS)], axis=0
        )
        q_blocks.append(
            jnp.where(block, jnp.concatenate([q_rows] * KV_HEADS, axis=1), 0.0).astype(BF16)
        )
    parts = []
    for d in range(docs):
        kv[2 * d].wait()
        scores = lax.dot_general(
            q_blocks[d], kbuf[d], (((1,), (1,)), ((), ())), preferred_element_type=F32
        ) * (HEAD_DIM ** (-0.5))
        keep = (col < len_ref[d]) | fresh_ok
        scores = jnp.where(keep, scores, -1e30)
        e = jnp.exp(scores - jnp.max(scores, -1, keepdims=True))
        probs = (e / jnp.sum(e, -1, keepdims=True)).astype(BF16)
        kv[2 * d + 1].wait()
        out = jnp.dot(probs, vbuf[d], preferred_element_type=F32)
        pieces = []
        for h in range(HEADS):
            k = h * NEW // per_kv
            pieces.append(out[h * NEW : (h + 1) * NEW, k * HEAD_DIM : (k + 1) * HEAD_DIM])
        parts.append(jnp.concatenate(pieces, axis=1))
    for copy in small[3:]:
        copy.wait()
    hid_all = hid[...].astype(F32)
    carried = jnp.concatenate([hid_all[:, d, :] + parts[d] for d in range(docs)], axis=0)
    carried_ref[...] = carried
    normed = carried * lax.rsqrt(jnp.mean(carried * carried, -1, keepdims=True) + 1e-05)
    cols[z, x, :, :width] = (normed * gain[...]).astype(BF16)
    cols[z, x, :, width:] = ext
    pl.semaphore_wait(barrier, len(greeted))

    def remote(src, dst, send, recv, device):
        return pltpu.make_async_remote_copy(
            src_ref=src, dst_ref=dst, send_sem=send, recv_sem=recv,
            device_id=device, device_id_type=MESH,
        )

    def whole(ref, send, recv):
        return remote(ref, ref, send, recv, partner)

    sides = ((0, -1), (1, 1))
    x_to = tuple(at(z, p, core) for p in x_next)
    x_from = x_next[::-1]
    middle = full // 256 * 128
    halves = (pl.ds(0, middle), pl.ds(middle, full - middle))

    def zg_copy(way, sign, leg, r):
        d = leg * RADIUS + r
        ref = cols.at[slab_of(sign * leg * RADIUS), x]
        if d == half:
            ref = ref.at[:, halves[way]]
        to = at(slab_of(-sign * r), x, core)
        return remote(ref, ref, zg_send.at[way, int(d == half)], zg_recv.at[way, d - 1], to)

    def send_leg(leg, way, sign):
        for r in range(RADIUS, 0, -1):
            zg_copy(way, sign, leg, r).start()

    def ways_of(d):
        return sides[:1] if d in (0, half) else sides

    def spread(d):
        for way, sign in ways_of(d):
            for side in range(2):
                ref = cols.at[slab_of(sign * d), x]
                remote(ref, ref, xf_send.at[0], xf_recv.at[d, side], x_to[side]).start()

    def relay(d):
        for side in range(2):
            count = len(ways_of(d))
            whole(cols.at[pl.ds(0, count), 0], xf_send.at[0], xf_recv.at[d, side]).wait_recv()
            for way, sign in ways_of(d):
                ref = cols.at[slab_of(sign * d), x_from[side], :, halves[side]]
                remote(ref, ref, xr_send.at[0], xr_recv.at[d], x_to[side]).start()

    def collect(d):
        count = len(ways_of(d))
        whole(cols.at[pl.ds(0, count), 0], xr_send.at[0], xr_recv.at[d]).wait_recv()
        for way, sign in ways_of(d):
            slab = slab_of(sign * d)
            rows[slab, 0] = jnp.concatenate(
                [cols[slab, j].astype(F32) for j in range(XS)], axis=0
            ).astype(BF16)
            d2_copy(way, sign, d).start()

    def d2_copy(way, sign, s):
        slab = slab_of(sign * s)
        return remote(rows.at[slab, 0], rows.at[slab, 1], d2_send.at[0], d2_recv.at[s], partner)

    def d2_wait(s, count):
        whole(rows.at[pl.ds(0, count), 1], d2_send.at[0], d2_recv.at[s]).wait_recv()

    nt = (((1,), (1,)), ((), ()))
    quarter = width // 4
    parts_of = (slice(0, width // 2), slice(width // 2, width))
    spans_of = (pl.ds(0, width // 2), pl.ds(width // 2, width // 2))

    def expert_rows(offsets):
        slabs = [slab_of(o) for o in offsets]
        lhs = jnp.concatenate([rows[w, k, :, :width] for w in slabs for k in range(2)], axis=0)
        tail = jnp.concatenate([rows[w, k, :, width:] for w in slabs for k in range(2)], axis=0)
        lanes = lax.broadcasted_iota(jnp.int32, tail.shape, 1)
        chosen = (lanes == mine_expert) | (lanes == mine_expert + EXPERTS)
        weight = jnp.sum(jnp.where(chosen, tail.astype(F32), 0.0), axis=-1, keepdims=True)
        gate = lax.dot_general(lhs, wg[...], nt, preferred_element_type=F32)
        up = lax.dot_general(lhs, wu[...], nt, preferred_element_type=F32)
        act = (jax.nn.silu(gate) * up * weight).astype(BF16)
        for c in range(4):
            cut = slice(c * quarter, (c + 1) * quarter)
            value = jnp.dot(act, wd[:, cut], preferred_element_type=F32)
            for i, w in enumerate(slabs):
                base = 2 * i * class_rows
                mine[w, :, cut] = value[base : base + class_rows]
                pair_out[w, :, cut] = value[base + class_rows : base + 2 * class_rows].astype(BF16)

    def pair_copy(way, d):
        slab = slab_of(-d if way == 0 else d)
        return remote(
            pair_out.at[slab], pair_in.at[slab], pr_send.at[0], pr_recv.at[d], partner
        )

    def pair_wait(d, count):
        whole(pair_in.at[pl.ds(0, count)], pr_send.at[0], pr_recv.at[d]).wait_recv()

    def next_rows(d):
        d2_wait(d, 2)
        expert_rows([d, -d])
        pair_copy(0, d).start()
        pair_copy(1, d).start()

    for way, sign in sides:
        send_leg(0, way, sign)
    spread(0)
    relay(0)
    legs = half // RADIUS
    waiting = [0]
    for leg in range(legs):
        near = leg * RADIUS
        landed = [near + r for r in range(RADIUS, 0, -1)]
        for d in landed:
            for way, sign in sides:
                zg_copy(way, sign, leg, d - near).wait_recv()
                if d == near + RADIUS and leg < legs - 1:
                    send_leg(leg + 1, way, sign)
            spread(d)
        for d in waiting:
            collect(d)
        for d in landed:
            relay(d)
        if leg == 1:
            for copy in w_copies:
                copy.wait()
            d2_wait(0, 1)
            expert_rows([0])
            pair_copy(0, 0).start()
        elif leg > 1:
            next_rows(near - RADIUS)
        waiting = landed
    next_rows(half - 2)
    for d in waiting:
        collect(d)
    next_rows(half - 3)

    def local_sum(d):
        pair_wait(d, len(ways_of(d)))
        for way, sign in ways_of(d):
            slab = slab_of(sign * d)
            total = mine[slab] + pair_in[slab].astype(F32)
            for j in range(XS):
                quad[slab, j] = total[j * ROWS : (j + 1) * ROWS]
            far_out[slab] = quad[slab, x_far].astype(BF16)
            for side in range(2):
                remote(
                    far_out.at[slab, :, spans_of[side]], far_in.at[slab, side],
                    far_send.at[0], far_recv.at[d], x_to[side],
                ).start()

    def neighbour_sum(d):
        count = len(ways_of(d))
        whole(far_out.at[pl.ds(0, count)], far_send.at[0], far_recv.at[d]).wait_recv()
        for way, sign in ways_of(d):
            slab = slab_of(sign * d)
            for side in range(2):
                col = x_next[side]
                here, there = parts_of[side], parts_of[1 - side]
                near_out[slab, side, :, here] = (
                    quad[slab, col, :, here] + far_in[slab, side].astype(F32)
                ).astype(BF16)
                near_out[slab, side, :, there] = quad[slab, col, :, there].astype(BF16)
                remote(
                    near_out.at[slab, side], near_in.at[slab, side],
                    near_send.at[0], near_recv.at[d], x_to[side],
                ).start()

    def zs_copy(way, sign, d):
        src, dst = z_out.at[way, d - 1], z_in.at[way, d - 1]
        if d == half:
            src, dst = src.at[:, spans_of[way]], dst.at[:, spans_of[way]]
        hop = d - (d - 1) // BACK * BACK
        to = at(slab_of(sign * hop), x, core)
        return remote(src, dst, zs_send.at[way, int(d == half)], zs_recv.at[way, d - 1], to)

    def column_sum(d):
        count = 2 * len(ways_of(d))
        whole(z_out.at[0, pl.ds(0, count)], near_send.at[0], near_recv.at[d]).wait_recv()
        for way, sign in ways_of(d):
            slab = slab_of(sign * d)
            taken = []
            if d % BACK == 0 and d < half:
                taken = [(w, s, d + r) for w, s in (sides if d == 0 else ((way, sign),)) for r in range(1, BACK + 1)]
            for w, s, e in taken:
                zs_copy(w, s, e).wait_recv()
            sums = []
            for h in range(2):
                cut = parts_of[h]
                total = quad[slab, x, :, cut]
                for side in range(2):
                    total = total + near_in[slab, side, :, cut].astype(F32)
                for w, s, e in taken:
                    if e < half or h == w:
                        total = total + z_in[w, e - 1, :, cut].astype(F32)
                sums.append(total)
            if d == 0:
                return jnp.concatenate(sums, axis=1)
            for w, s in sides if d == half else ((way, sign),):
                for h in range(2):
                    if d < half or h == w:
                        z_out[w, d - 1, :, parts_of[h]] = sums[h].astype(BF16)
                zs_copy(w, s, d).start()

    def last_rows(d):
        d2_wait(d, 1)
        expert_rows([d])
        pair_copy(0, d).start()

    local_sum(half - 2)
    last_rows(half)
    local_sum(half - 3)
    next_rows(half - 1)
    local_sum(half)
    neighbour_sum(half - 2)
    local_sum(half - 1)
    neighbour_sum(half - 3)
    local_sum(half - 4)
    neighbour_sum(half)
    column_sum(half - 2)
    next_rows(half - 5)
    neighbour_sum(half - 1)
    column_sum(half - 3)
    local_sum(half - 5)
    neighbour_sum(half - 4)
    column_sum(half)
    next_rows(half - 7)
    local_sum(half - 6)
    neighbour_sum(half - 5)
    column_sum(half - 1)
    local_sum(half - 7)
    neighbour_sum(half - 6)
    local_sum(0)
    column_sum(half - 4)
    neighbour_sum(half - 7)
    column_sum(half - 5)
    neighbour_sum(0)
    column_sum(half - 6)
    column_sum(half - 7)
    result = carried_ref[...] + column_sum(0)
    for d in range(DOC_DEV):
        for t in range(NEW):
            r = d * NEW + t
            out_ref[t, d : d + 1, :] = result[r : r + 1].astype(BF16)

    whole(cols.at[:, pl.ds(0, 2)], xf_send.at[0], xf_recv.at[0, 0]).wait_send()
    whole(cols.at[:, 0], xr_send.at[0], xr_recv.at[0]).wait_send()
    for way in range(2):
        whole(cols.at[pl.ds(0, half - 1), 0], zg_send.at[way, 0], zg_recv.at[0, 0]).wait_send()
        whole(cols.at[0, 0, :, halves[way]], zg_send.at[way, 1], zg_recv.at[0, 0]).wait_send()
        whole(z_out.at[0, pl.ds(0, half - 1)], zs_send.at[way, 0], zs_recv.at[0, 0]).wait_send()
        whole(z_out.at[0, 0, :, spans_of[way]], zs_send.at[way, 1], zs_recv.at[0, 0]).wait_send()
    whole(far_out, far_send.at[0], far_recv.at[0]).wait_send()
    whole(near_out, near_send.at[0], near_recv.at[0]).wait_send()
    whole(rows.at[:, 0], d2_send.at[0], d2_recv.at[0]).wait_send()
    whole(pair_out, pr_send.at[0], pr_recv.at[0]).wait_send()


def per_device(
    hidden_in, norm_gain, queries, new_keys, new_values, cache_keys, cache_values,
    lengths, routes, gate_logits, w_gate, w_up, w_down,
):
    nz = lax.axis_size("dp") // (XS * CORES)
    half = nz // 2
    width = hidden_in.shape[2]
    docs, cache_len, kv_width = cache_keys.shape
    hidden = w_gate.shape[0]
    full = width + EXT
    class_rows = XS * ROWS
    vmem = pl.BlockSpec(memory_space=pltpu.VMEM)
    smem = pl.BlockSpec(memory_space=pltpu.SMEM)
    hbm = pl.BlockSpec(memory_space=pl.ANY)
    dma = pltpu.SemaphoreType.DMA
    return pl.pallas_call(
        functools.partial(layer_kernel, nz),
        name="layer",
        out_shape=jax.ShapeDtypeStruct(hidden_in.shape, BF16),
        in_specs=[hbm] * 7 + [smem] * 3 + [hbm] * 3,
        out_specs=vmem,
        scratch_shapes=[
            pltpu.VMEM(hidden_in.shape, BF16),
            pltpu.VMEM((1, width), F32),
            pltpu.VMEM(queries.shape, BF16),
            pltpu.VMEM(new_keys.shape, BF16),
            pltpu.VMEM(new_values.shape, BF16),
            pltpu.VMEM((docs, cache_len + TAIL, kv_width), BF16),
            pltpu.VMEM((docs, cache_len + TAIL, kv_width), BF16),
            pltpu.VMEM((hidden, width), BF16),
            pltpu.VMEM((hidden, width), BF16),
            pltpu.VMEM((hidden, width), BF16),
            pltpu.VMEM((ROWS, width), F32),
            pltpu.VMEM((nz, XS, ROWS, full), BF16),
            pltpu.VMEM((nz, 2, class_rows, full), BF16),
            pltpu.VMEM((nz, class_rows, width), F32),
            pltpu.VMEM((nz, class_rows, width), BF16),
            pltpu.VMEM((nz, class_rows, width), BF16),
            pltpu.VMEM((nz, XS, ROWS, width), F32),
            pltpu.VMEM((nz, ROWS, width), BF16),
            pltpu.VMEM((nz, 2, ROWS, width // 2), BF16),
            pltpu.VMEM((nz, 2, ROWS, width), BF16),
            pltpu.VMEM((nz, 2, ROWS, width), BF16),
            pltpu.VMEM((2, half, ROWS, width), BF16),
            pltpu.VMEM((2, half, ROWS, width), BF16),
            dma((5,)), dma((docs, 2)), dma((3,)),
            dma((2, 2)), dma((2, half)),
            dma((1,)), dma((half + 1, 2)),
            dma((1,)), dma((half + 1,)),
            dma((1,)), dma((half + 1,)),
            dma((1,)), dma((half + 1,)),
            dma((1,)), dma((half + 1,)),
            dma((1,)), dma((half + 1,)),
            dma((2, 2)), dma((2, half)),
        ],
        compiler_params=pltpu.CompilerParams(
            collective_id=0, has_side_effects=True, vmem_limit_bytes=56 * 1024 * 1024
        ),
    )(
        hidden_in, norm_gain.reshape(1, width), queries, new_keys, new_values, cache_keys,
        cache_values, lengths, routes, gate_logits, w_gate, w_up, w_down,
    )


def solution(mesh):
    in_specs = (
        P(None, ("grp", "dp"), None),
        P(),
        P(None, ("grp", "dp"), None),
        P(None, ("grp", "dp"), None),
        P(None, ("grp", "dp"), None),
        P(("grp", "dp"), None, None),
        P(("grp", "dp"), None, None),
        P(("grp", "dp")),
        P(None, ("grp", "dp"), None),
        P(None, ("grp", "dp"), None),
        P("dp", None),
        P("dp", None),
        P("dp", None),
    )
    out_specs = P(None, ("grp", "dp"), None)
    return jax.shard_map(
        per_device, mesh=mesh, in_specs=in_specs, out_specs=out_specs, check_vma=False
    )
```
